128 devices in a mesh: comm: 8 (over y, x_lo), dom: 16 (over z, x_hi, core).
Axes of the slice: x: 4 (x_hi: 2, x_lo: 2; x = x_hi * 2 + x_lo), y: 4, z: 4, core: 2. Of those that a mesh axis runs over, the one named last changes fastest.
Arguments:
- initial: bfloat16 [65536, 512], P(('comm', 'dom')), may hold values from -6 to 6
- held_cross: bfloat16 [65536, 512], P(('comm', 'dom')), may hold values from -6 to 6
- weights: bfloat16 [3, 512, 512], replicated, may hold values from -0.25 to 0.25
- need_rows: int32 [8, 16, 16, 1], P('comm', 'dom'), may hold values from 0 to 3
- tiles: bfloat16 [8, 16, 192, 128, 128], P('comm', 'dom'), may hold values from -1 to 1
- tile_scale: float32 [8, 16, 192], P('comm', 'dom'), may hold values from 0.01 to 0.1
- tile_src: int32 [8, 16, 192], P('comm', 'dom'), may hold values from 0 to 19, as said below
- tile_dst: int32 [8, 16, 192], P('comm', 'dom'), may hold values from 0 to 3
- tile_count: int32 [8, 16], P('comm', 'dom'), may hold values from 20 to 192
- cross_need: int32 [8, 16, 8, 2], P('comm', 'dom'), may hold values from 0 to 3
- cross_tiles: bfloat16 [8, 16, 64, 128, 128], P('comm', 'dom'), may hold values from -1 to 1
- cross_scale: float32 [8, 16, 64], P('comm', 'dom'), may hold values from 0.03 to 0.3
- cross_src: int32 [8, 16, 64], P('comm', 'dom'), may hold values from 0 to 15, as said below
- cross_dst: int32 [8, 16, 64], P('comm', 'dom'), may hold values from 0 to 3
Outputs:
- output: bfloat16 [65536, 512], P(('comm', 'dom'))
- refreshed: bfloat16 [65536, 512], P(('comm', 'dom'))
The draws below stay inside these ranges and needn't reach their ends.
Inputs may be any that keep to these rules, and one draw needn't show every extreme that they name: `tile_src`: a partition's first 20 tiles name every in-community source index once. `cross_src`: a partition's first 16 cross tiles name every cross source index once.
All inputs are finite; a program needn't handle non-finite values.
Results may differ from the reference program's by a relative error of at most 0.0071.
Values may be sent and summed in bfloat16 or wider, within the bound.
A program may use at most 128 MiB of HBM per device.

```python
import math
import jax
import jax.numpy as jnp
from jax import lax

D = 512
BLOCK = 128
BLK_DEV = 4
SEND_CAP = 1
CROSS_CAP = 2
TILES_DEV = 192
XTILES_DEV = 64
SOURCES = 20
XSOURCES = 16
NODES = 65536
N_COMM = 8
N_DOM = 16


def covering_sources(key, count, sources):
    devices = N_COMM * N_DOM
    first, second = jax.random.split(jax.random.fold_in(key, 7))
    perm_keys = jax.random.split(first, devices)
    leading = jax.vmap(lambda item: jax.random.permutation(item, sources))(perm_keys).astype(jnp.int32)
    rest = jax.random.randint(second, (devices, count - sources), 0, sources).astype(jnp.int32)
    return jnp.concatenate([leading, rest], 1).reshape(N_COMM, N_DOM, count)


def draw_tile_src(key, part):
    return covering_sources(key, TILES_DEV, SOURCES)


def draw_cross_src(key, part):
    return covering_sources(jax.random.fold_in(key, 11), XTILES_DEV, XSOURCES)


def draw_tile_count(key, part):
    devices = N_COMM * N_DOM
    first, second = jax.random.split(jax.random.fold_in(key, 3))
    level = jax.random.randint(first, (devices,), 0, 64).astype(jnp.int32)
    count = SOURCES + (TILES_DEV - SOURCES) * level * level * level // 250047
    chosen = jax.random.randint(second, (), 0, devices)
    count = jnp.where(jnp.arange(devices, dtype=jnp.int32) == chosen, TILES_DEV, count)
    return count.reshape(N_COMM, N_DOM).astype(jnp.int32)


def with_ends(values, stream_key, smallest, top_value):
    index_at = [jax.random.randint(jax.random.fold_in(stream_key, axis), (), 0, length) for axis, length in enumerate(values.shape)]
    longest = values.shape.index(max(values.shape))
    neighbour = index_at[:longest] + [(index_at[longest] + 1) % values.shape[longest]] + index_at[longest + 1:]
    return values.at[tuple(index_at)].set(smallest).at[tuple(neighbour)].set(top_value)


def shard_levels(key, dims, shards, smallest, largest):
    loudness = 1.0
    for position, shards_of in shards:
        draws = jax.random.uniform(jax.random.fold_in(jax.random.fold_in(key, 6), position), (shards_of,), jnp.float32, smallest / len(shards), largest / len(shards))
        loudness = loudness * jnp.repeat(jnp.exp(draws), dims[position] // shards_of).reshape((-1,) + (1,) * (len(dims) - 1 - position))
    return loudness


def noise(own_key, dims, scale, limit, shards=(), kind=jnp.bfloat16):
    values = jax.random.normal(own_key, dims, jnp.float32) * scale
    if len(shards) > 0:
        values = shard_levels(own_key, dims, shards, -0.22, 0.18) * values
    return jnp.clip(values, min=-limit, max=limit).astype(kind)


def setup_inputs(seed: int = 0) -> dict:
    key_list = jax.random.split(jax.random.key(seed), 15)
    initial = noise(key_list[0], (NODES, D), 1.0, 6.0, ((0, 128),))
    held_cross = noise(key_list[1], (NODES, D), 1.0, 6.0, ((0, 128),))
    weights = noise(key_list[2], (3, D, D), D ** -0.5, 0.25)
    need_rows = with_ends(jax.random.randint(key_list[3], (N_COMM, N_DOM, N_DOM, SEND_CAP), 0, BLK_DEV), jax.random.fold_in(key_list[3], 1), 0, BLK_DEV - 1).astype(jnp.int32)
    tiles = jnp.clip(jax.random.uniform(key_list[4], (N_COMM, N_DOM, TILES_DEV, BLOCK, BLOCK), jnp.float32, -1.0, 1.0) * shard_levels(key_list[4], (N_COMM, N_DOM, TILES_DEV, BLOCK, BLOCK), ((0, 8), (1, 16)), -0.4, 0.0), -1.0, 1.0).astype(jnp.bfloat16)
    tile_scale = jnp.clip(jnp.exp(math.log(0.1) - 2.3025851 * jax.random.uniform(key_list[5], (N_COMM, N_DOM, TILES_DEV), jnp.float32) ** shard_levels(key_list[5], (N_COMM, N_DOM, TILES_DEV), ((0, 8), (1, 16)), -0.2, 0.2)), 0.01, 0.1)
    tile_src = draw_tile_src(jax.random.fold_in(key_list[14], 71), 0)
    tile_dst = with_ends(jax.random.randint(key_list[7], (N_COMM, N_DOM, TILES_DEV), 0, BLK_DEV), jax.random.fold_in(key_list[7], 1), 0, BLK_DEV - 1).astype(jnp.int32)
    tile_count = draw_tile_count(jax.random.fold_in(key_list[14], 71), 0)
    cross_need = with_ends(jax.random.randint(key_list[9], (N_COMM, N_DOM, N_COMM, CROSS_CAP), 0, BLK_DEV), jax.random.fold_in(key_list[9], 1), 0, BLK_DEV - 1).astype(jnp.int32)
    cross_tiles = jnp.clip(jax.random.uniform(key_list[10], (N_COMM, N_DOM, XTILES_DEV, BLOCK, BLOCK), jnp.float32, -1.0, 1.0) * shard_levels(key_list[10], (N_COMM, N_DOM, XTILES_DEV, BLOCK, BLOCK), ((0, 8), (1, 16)), -0.4, 0.0), -1.0, 1.0).astype(jnp.bfloat16)
    cross_scale = jnp.clip(jnp.exp(math.log(0.3) - 2.3025852 * jax.random.uniform(key_list[11], (N_COMM, N_DOM, XTILES_DEV), jnp.float32) ** shard_levels(key_list[11], (N_COMM, N_DOM, XTILES_DEV), ((0, 8), (1, 16)), -0.2, 0.2)), 0.03, 0.3)
    cross_src = draw_cross_src(jax.random.fold_in(key_list[14], 71), 0)
    cross_dst = with_ends(jax.random.randint(key_list[13], (N_COMM, N_DOM, XTILES_DEV), 0, BLK_DEV), jax.random.fold_in(key_list[13], 1), 0, BLK_DEV - 1).astype(jnp.int32)
    return dict(initial=initial, held_cross=held_cross, weights=weights, need_rows=need_rows, tiles=tiles, tile_scale=tile_scale, tile_src=tile_src, tile_dst=tile_dst, tile_count=tile_count, cross_need=cross_need, cross_tiles=cross_tiles, cross_scale=cross_scale, cross_src=cross_src, cross_dst=cross_dst)


ALPHA = 0.1
LAMBDA = 0.5


def dense_layer(total, initial, weight, level):
    beta = math.log(LAMBDA / level + 1.0)
    mixed = (1.0 - ALPHA) * total + ALPHA * initial.astype(jnp.float32)
    rounded = mixed.astype(jnp.bfloat16)
    turned = jnp.dot(rounded, weight, preferred_element_type=jnp.float32)
    return jax.nn.relu((1.0 - beta) * mixed + beta * turned).astype(jnp.bfloat16)


def assemble(tiles, scales, src_idx, dst_idx, live, blocks, sources):
    alive = jnp.arange(tiles.shape[0], dtype=jnp.int32) < live
    factor = jnp.where(alive, scales, jnp.zeros_like(scales))
    into = (dst_idx[:, None] == jnp.arange(blocks, dtype=jnp.int32)[None, :]).astype(jnp.float32) * factor[:, None]
    where = (src_idx[:, None] == jnp.arange(sources, dtype=jnp.int32)[None, :]).astype(jnp.float32)
    dense = jnp.einsum("tb,ts,tij->bisj", into, where, tiles.astype(jnp.float32), precision=lax.Precision.HIGHEST)
    return dense.reshape(blocks * BLOCK, sources * BLOCK).astype(jnp.bfloat16)


def reference(initial, held_cross, weights, need_rows, tiles, tile_scale, tile_src, tile_dst, tile_count, cross_need, cross_tiles, cross_scale, cross_src, cross_dst):
    devices = N_COMM * N_DOM
    width = initial.shape[1]
    ident = jnp.arange(devices, dtype=jnp.int32)

    def flatten(array):
        return array.reshape((devices,) + array.shape[2:])

    def inner(hidden):
        table = hidden.reshape(devices * BLK_DEV, BLOCK, width)

        def single(inputs):
            device, need, tile, scale, source, target, live = inputs
            group = device // N_DOM
            own = lax.dynamic_slice_in_dim(table, device * BLK_DEV, BLK_DEV, 0)
            index = (group * N_DOM + jnp.arange(N_DOM, dtype=jnp.int32)[:, None]) * BLK_DEV + need
            stacked = jnp.concatenate([own, table[index.reshape(-1)]], 0).reshape(SOURCES * BLOCK, width)
            matrix = assemble(tile, scale, source, target, live, BLK_DEV, SOURCES)
            return jnp.dot(matrix, stacked, preferred_element_type=jnp.float32)

        result = lax.map(single, (ident, flatten(need_rows), flatten(tiles), flatten(tile_scale), flatten(tile_src), flatten(tile_dst), tile_count.reshape(devices)))
        return result.reshape(devices * BLK_DEV * BLOCK, width)

    def across(hidden):
        table = hidden.reshape(devices * BLK_DEV, BLOCK, width)

        def single(inputs):
            device, need, tile, scale, source, target = inputs
            member = device % N_DOM
            index = (jnp.arange(N_COMM, dtype=jnp.int32)[:, None] * N_DOM + member) * BLK_DEV + need
            stacked = table[index.reshape(-1)].reshape(XSOURCES * BLOCK, width)
            matrix = assemble(tile, scale, source, target, XTILES_DEV, BLK_DEV, XSOURCES)
            return jnp.dot(matrix, stacked, preferred_element_type=jnp.float32)

        result = lax.map(single, (ident, flatten(cross_need), flatten(cross_tiles), flatten(cross_scale), flatten(cross_src), flatten(cross_dst)))
        return result.reshape(devices * BLK_DEV * BLOCK, width)

    hidden = initial
    for level in (1, 2):
        total = inner(hidden) + held_cross.astype(jnp.float32)
        hidden = dense_layer(total, initial, weights[level - 1], level)
    refreshed = across(hidden).astype(jnp.bfloat16)
    total = inner(hidden) + refreshed.astype(jnp.float32)
    output = dense_layer(total, initial, weights[2], 3)
    return output, refreshed
```

```python
import functools
import math

import jax
import jax.numpy as jnp
from jax import lax
from jax.experimental import pallas as pl
from jax.experimental.pallas import tpu as pltpu
from jax.sharding import PartitionSpec as P

BLOCK = 128
D = 512
ROWS = 512
TILES = 192
XTILES = 64
SOURCES = 20
XSOURCES = 16
ALPHA = 0.1
LAMBDA = 0.5
MESH = pl.DeviceIdType.MESH
BF = jnp.bfloat16
F32 = jnp.float32
I32 = jnp.int32
OWN, ANT = 0, 1


def pair(i):
    return pl.ds(i * 2, 2)


def chain_tables(key_ref, tbl_ref, halves, none, row):
    iota0 = lax.broadcasted_iota(I32, (BLOCK, BLOCK), 0)
    iota1 = lax.broadcasted_iota(I32, (BLOCK, BLOCK), 1)
    last = jnp.full((1, BLOCK), -1, I32)
    prev = [jnp.full((1, BLOCK), -1, I32) for _ in range(halves)]
    for h in range(halves):
        down = jnp.broadcast_to(key_ref[0:1, h * BLOCK : (h + 1) * BLOCK], (BLOCK, BLOCK)).T
        who = iota0 + h * BLOCK
        hit = jnp.where(down == iota1, who, -1)
        last = jnp.maximum(last, jnp.max(hit, axis=0, keepdims=True))
        for j in range(h, halves):
            across = jnp.broadcast_to(key_ref[0:1, j * BLOCK : (j + 1) * BLOCK], (BLOCK, BLOCK))
            same = jnp.logical_and(down == across, who < iota1 + j * BLOCK)
            prev[j] = jnp.maximum(prev[j], jnp.max(jnp.where(same, who, -1), axis=0, keepdims=True))
    tbl_ref[row : row + 1, 0:BLOCK] = jnp.where(last < 0, none, last)
    for j in range(halves):
        tbl_ref[row : row + 1, (j + 1) * BLOCK : (j + 2) * BLOCK] = jnp.where(prev[j] < 0, none, prev[j])


def kernel(
    init_hbm,
    held_hbm,
    weights_hbm,
    need_ref,
    tiles_hbm,
    scale_ref,
    src_ref,
    dst_ref,
    count_ref,
    xneed_ref,
    xtiles_hbm,
    xscale_ref,
    xsrc_ref,
    xdst_ref,
    out_ref,
    ref_ref,
    init,
    held,
    weights,
    tiles,
    slots,
    adj,
    xadj,
    acc,
    xacc,
    rounded,
    hbuf,
    rb,
    ant0,
    ant1,
    ant2,
    xf,
    zf,
    nbt,
    gb,
    cr,
    yf,
    gx,
    rq,
    reqs,
    xreqs,
    reqs_s,
    xreqs_s,
    keys,
    tbl,
    tbl_s,
    lsem,
    ssem,
    qsem,
    xs,
    as_,
    zs,
    rs,
    ns,
    ys,
    cs,
):
    comm = lax.axis_index("comm")
    dom = lax.axis_index("dom")
    y, xl = comm // 2, comm % 2
    z, xh, c = dom // 4, (dom // 2) % 2, dom % 2
    x = xh * 2 + xl

    def dev(px, py, pz, pc):
        return (py * 2 + px % 2, pz * 4 + (px // 2) * 2 + pc)

    xp, xm = (x + 1) % 4, (x + 3) % 4
    xnb = xh * 2 + (1 - xl)
    xot = (x + 3 + 2 * xl) % 4
    zp, zm, z2 = (z + 1) % 4, (z + 3) % 4, (z + 2) % 4
    yp, ym, y2 = (y + 1) % 4, (y + 3) % 4, (y + 2) % 4

    ant = (ant0, ant1, ant2)

    loads = {}

    def load(name, src, dst, i):
        loads[name] = pltpu.make_async_copy(src, dst, lsem.at[i])
        loads[name].start()

    load("init", init_hbm, init, 0)
    load("tiles0", tiles_hbm.at[pl.ds(0, 96)], tiles.at[pl.ds(0, 96)], 1)
    load("tiles1", tiles_hbm.at[pl.ds(96, 96)], tiles.at[pl.ds(96, 96)], 2)
    load("held", held_hbm, held, 3)
    load("weights", weights_hbm, weights, 4)

    barrier = pltpu.get_barrier_semaphore()
    peers = [
        dev(xp, y, z, c),
        dev(xm, y, z, c),
        dev(x, y, z, 1 - c),
        dev(x, y, zp, 0),
        dev(x, y, zp, 1),
        dev(x, y, zm, 0),
        dev(x, y, zm, 1),
        dev(x, y, z2, 0),
        dev(x, y, z2, 1),
        dev(x, yp, z, c),
        dev(x, ym, z, c),
        dev(x, y2, z, c),
    ]
    for peer in peers:
        pl.semaphore_signal(barrier, inc=1, device_id=peer, device_id_type=MESH)
    rq[0:1, 0:16] = need_ref[...]
    rq[1:2, 0:16] = xneed_ref[...]
    loads["init"].wait()
    pl.semaphore_wait(barrier, len(peers))

    sent = []

    def send(src, dst, sem, device):
        copy = pltpu.make_async_remote_copy(
            src_ref=src,
            dst_ref=dst,
            send_sem=ssem.at[len(sent)],
            recv_sem=sem,
            device_id=device,
            device_id_type=MESH,
        )
        copy.start()
        sent.append(copy)

    def arrived(dst, sem):
        pltpu.make_async_remote_copy(
            src_ref=dst,
            dst_ref=dst,
            send_sem=ssem.at[0],
            recv_sem=sem,
            device_id=dev(x, y, z, 1 - c),
            device_id_type=MESH,
        ).wait_recv()

    def x_first(e, table, half):
        if half == 0:
            for k in range(2):
                send(table.at[k], xf.at[e, 0, k], xs.at[e, 0, k], dev(xp, y, z, c))
        else:
            for k in range(2):
                send(table.at[2 + k], xf.at[e, 1, k], xs.at[e, 1, k], dev(xm, y, z, c))

    def x_forward(e, k):
        arrived(xf.at[e, 0, k], xs.at[e, 0, k])
        send(xf.at[e, 0, k], ant[e].at[k], as_.at[e, k], dev(xp, y, z, c))
        arrived(xf.at[e, 1, k], xs.at[e, 1, k])
        send(xf.at[e, 1, k], ant[e].at[2 + k], as_.at[e, 2 + k], dev(xm, y, z, c))

    def part(pz, ty, pc):
        return pz * 4 + (xh if ty == OWN else 1 - xh) * 2 + pc

    def z_send(e, ty, table):
        p = part(z, ty, c)

        def gather(g, pz, pc):
            want = reqs_s[pz * 2 + pc, 0, p]
            gb[ty, g] = table[want]
            return gb.at[ty, g]

        mine = rb.at[e, p]
        send(gather(0, z2, 0), zf.at[e, 0, ty], zs.at[e, 0, ty], dev(x, y, zp, c))
        send(gather(1, z2, 1), zf.at[e, 1, ty], zs.at[e, 1, ty], dev(x, y, zm, c))
        send(gather(2, zp, 0), mine, rs.at[e, 0, ty, c], dev(x, y, zp, 0))
        send(gather(3, zm, 0), mine, rs.at[e, 1, ty, c], dev(x, y, zm, 0))
        send(gather(4, zp, 1), mine, rs.at[e, 0, ty, c], dev(x, y, zp, 1))
        send(gather(5, zm, 1), mine, rs.at[e, 1, ty, c], dev(x, y, zm, 1))
        send(gather(6, z, 1 - c), mine, rs.at[e, 3, ty, 0], dev(x, y, z, 1 - c))
        want = reqs_s[z * 2 + c, 0, p]
        rb[e, p] = table[want]

    def z_forward(e, ty):
        arrived(zf.at[e, 0, ty], zs.at[e, 0, ty])
        send(zf.at[e, 0, ty], rb.at[e, part(zm, ty, c)], rs.at[e, 2, ty, c], dev(x, y, zp, 0))
        arrived(zf.at[e, 1, ty], zs.at[e, 1, ty])
        send(zf.at[e, 1, ty], rb.at[e, part(zp, ty, c)], rs.at[e, 2, ty, c], dev(x, y, zm, 1))

    def dot_into(total, lhs, rhs, first=False):
        @pl.loop(0, 2)
        def _(n):
            cols = pl.ds(pl.multiple_of(n * 256, 256), 256)
            value = jnp.dot(lhs[...], rhs[:, :, cols].reshape(256, 256), preferred_element_type=F32)
            if first:
                total[:, cols] = value
            else:
                total[:, cols] += value

    def dot_own(table):
        dot_into(acc, adj.at[0], table.at[pl.ds(0, 2)], first=True)
        dot_into(acc, adj.at[1], table.at[pl.ds(2, 2)])

    def dot_pair(e, ty, key):
        pz = (zm, zp, z2, z)[key]
        if key == 3:
            arrived(rb.at[e, part(z, ty, 1 - c)], rs.at[e, 3, ty, 0])
        else:
            for pc in range(2):
                arrived(rb.at[e, part(pz, ty, pc)], rs.at[e, key, ty, pc])
        j = pz * 2 + (xh if ty == OWN else 1 - xh)
        dot_into(acc, adj.at[2 + j], rb.at[e, pair(j)])

    def drain():
        for copy in sent:
            copy.wait_send()
        sent.clear()

    def layer(level, added, target, after=lambda half: None, blocks=True):
        beta = math.log(LAMBDA / level + 1.0)
        for half in range(2):
            rows = pl.ds(half * 256, 256)
            total = acc[rows, :] + added[rows, :].astype(F32)
            mixed = (1.0 - ALPHA) * total + ALPHA * init[2 * half : 2 * half + 2].reshape(256, D).astype(F32)
            acc[rows, :] = mixed
            rounded[rows, :] = mixed.astype(BF)
            for n in range(2):
                cols = pl.ds(n * 256, 256)
                turned = jnp.dot(rounded[rows, :], weights[level - 1, :, cols], preferred_element_type=F32)
                done = jax.nn.relu((1.0 - beta) * acc[rows, cols] + beta * turned).astype(BF)
                if blocks:
                    target[2 * half : 2 * half + 2, :, cols] = done.reshape(2, BLOCK, 256)
                else:
                    target[rows, cols] = done
            after(half)

    x_first(0, init, 0)
    x_first(0, init, 1)
    for pz in (zp, zm, z2):
        for pc in range(2):
            send(rq, reqs.at[z * 2 + c], qsem.at[z * 2 + c], dev(x, y, pz, pc))
    send(rq, reqs.at[z * 2 + c], qsem.at[z * 2 + c], dev(x, y, z, 1 - c))
    for py in (yp, ym, y2):
        send(rq, xreqs.at[y], qsem.at[8 + y], dev(x, py, z, c))
    reqs[z * 2 + c] = rq[...]
    xreqs[y] = rq[...]

    keys[...] = jnp.full((8, 256), -1, I32)
    live = count_ref[0, 0]
    at = lax.broadcasted_iota(I32, (1, TILES), 1)
    keys[0:1, 0:TILES] = jnp.where(at < live, dst_ref[...] * SOURCES + src_ref[...], -1)
    chain_tables(keys, tbl, 2, TILES, 0)
    keys[0:1, 0:256] = jnp.full((1, 256), -1, I32)
    keys[0:1, 0:XTILES] = xdst_ref[...] * XSOURCES + xsrc_ref[...]
    chain_tables(keys, tbl, 1, TILES, 1)
    copy_tbl = pltpu.make_async_copy(tbl, tbl_s, lsem.at[5])
    copy_tbl.start()
    slots[TILES] = jnp.zeros((BLOCK, BLOCK), F32)

    for pz in (zp, zm, z2):
        for pc in range(2):
            arrived(reqs.at[pz * 2 + pc], qsem.at[pz * 2 + pc])
    arrived(reqs.at[z * 2 + 1 - c], qsem.at[z * 2 + 1 - c])
    copy_req = pltpu.make_async_copy(reqs, reqs_s, lsem.at[6])
    copy_req.start()
    copy_req.wait()
    z_send(0, OWN, init)
    for py in (yp, ym, y2):
        arrived(xreqs.at[py], qsem.at[8 + py])
    copy_xreq = pltpu.make_async_copy(xreqs, xreqs_s, lsem.at[7])
    copy_xreq.start()
    copy_xreq.wait()
    copy_tbl.wait()

    def chain(tile_ref, scales, row, start, stop):
        @pl.loop(start, stop)
        def _(t):
            before = tbl_s[row, BLOCK + t]
            slots[t] = slots[before] + scales[0, t] * tile_ref[t].astype(F32)

    def place(target, row, sources):
        @pl.loop(0, sources // 2)
        def _(s2):
            for b in range(4):
                for s in range(2):
                    final = tbl_s[row, b * sources + s2 * 2 + s]
                    target[s2, b * BLOCK : (b + 1) * BLOCK, s * BLOCK : (s + 1) * BLOCK] = slots[final].astype(BF)

    loads["tiles0"].wait()
    chain(tiles, scale_ref, 0, 0, 48)
    x_forward(0, 0)
    chain(tiles, scale_ref, 0, 48, 96)
    x_forward(0, 1)
    loads["tiles1"].wait()
    chain(tiles, scale_ref, 0, 96, 144)
    z_forward(0, OWN)
    chain(tiles, scale_ref, 0, 144, 192)
    load("xtiles", xtiles_hbm, tiles.at[pl.ds(0, XTILES)], 8)
    place(adj, 0, SOURCES)
    dot_own(init)
    for k in range(4):
        arrived(ant[0].at[k], as_.at[0, k])
    z_send(0, ANT, ant[0])
    dot_pair(0, OWN, 3)
    dot_pair(0, OWN, 0)
    dot_pair(0, OWN, 1)
    z_forward(0, ANT)
    dot_pair(0, OWN, 2)
    loads["xtiles"].wait()
    chain(tiles, xscale_ref, 1, 0, XTILES)
    place(xadj, 1, XSOURCES)
    loads["held"].wait()
    loads["weights"].wait()
    dot_pair(0, ANT, 3)
    dot_pair(0, ANT, 0)
    dot_pair(0, ANT, 1)
    dot_pair(0, ANT, 2)
    drain()
    layer(1, held, hbuf.at[0], lambda half: x_first(1, hbuf.at[0], half))

    h1 = hbuf.at[0]
    z_send(1, OWN, h1)
    dot_own(h1)
    x_forward(1, 0)
    x_forward(1, 1)
    z_forward(1, OWN)
    dot_pair(1, OWN, 3)
    dot_pair(1, OWN, 0)
    dot_pair(1, OWN, 1)
    for k in range(4):
        arrived(ant[1].at[k], as_.at[1, k])
    z_send(1, ANT, ant[1])
    dot_pair(1, OWN, 2)
    dot_pair(1, ANT, 3)
    z_forward(1, ANT)
    dot_pair(1, ANT, 0)
    dot_pair(1, ANT, 1)
    dot_pair(1, ANT, 2)
    drain()

    h2 = hbuf.at[1]

    def x_table(half):
        for k in range(2 * half, 2 * half + 2):
            send(h2.at[k], nbt.at[k], ns.at[k], dev(xnb, y, z, c))

    def x_table_forward(k):
        arrived(nbt.at[k], ns.at[k])
        send(nbt.at[k], ant[2].at[k], as_.at[2, k], dev(xot, y, z, c))

    def group(py, ty):
        return py * 2 + (xl if ty == OWN else 1 - xl)

    def y_send(ty, table):
        me = group(y, ty)

        def gather(g, py, k):
            want = xreqs_s[py, 1, me * 2 + k]
            gx[ty, g] = table[want]

        gather(0, y2, 0)
        gather(1, y2, 1)
        send(gx.at[ty, 0], yf.at[0, ty], ys.at[0, ty], dev(x, yp, z, c))
        send(gx.at[ty, 1], yf.at[1, ty], ys.at[1, ty], dev(x, ym, z, c))
        mine = cr.at[pair(me)]
        for i, py in enumerate((yp, ym)):
            gather(2 + 2 * i, py, 0)
            gather(3 + 2 * i, py, 1)
            send(gx.at[ty, pair(1 + i)], mine, cs.at[i, ty], dev(x, py, z, c))
        for k in range(2):
            want = xreqs_s[y, 1, me * 2 + k]
            cr[me * 2 + k] = table[want]

    def y_forward(ty):
        arrived(yf.at[0, ty], ys.at[0, ty])
        send(yf.at[0, ty], cr.at[group(ym, ty) * 2], cs.at[2, ty], dev(x, yp, z, c))
        arrived(yf.at[1, ty], ys.at[1, ty])
        send(yf.at[1, ty], cr.at[group(yp, ty) * 2 + 1], cs.at[3, ty], dev(x, ym, z, c))

    layer(2, held, h2, x_table)
    z_send(2, OWN, h2)
    y_send(OWN, h2)
    dot_own(h2)
    x_table_forward(0)
    z_forward(2, OWN)
    y_forward(OWN)
    x_table_forward(1)
    dot_pair(2, OWN, 3)
    x_table_forward(2)
    dot_pair(2, OWN, 0)
    dot_pair(2, OWN, 1)
    x_table_forward(3)
    y_send(ANT, nbt)

    def cross_dot(ty, key, first=False):
        py = (ym, yp, y2, y)[key]
        g = group(py, ty)
        if key < 2:
            arrived(cr.at[pair(g)], cs.at[key, ty])
        if key == 2:
            arrived(cr.at[g * 2], cs.at[2, ty])
            arrived(cr.at[g * 2 + 1], cs.at[3, ty])
        dot_into(xacc, xadj.at[g], cr.at[pair(g)], first)

    cross_dot(OWN, 3, first=True)
    cross_dot(ANT, 3)
    dot_pair(2, OWN, 2)
    cross_dot(OWN, 0)
    cross_dot(OWN, 1)
    for k in range(4):
        arrived(ant[2].at[k], as_.at[2, k])
    z_send(2, ANT, ant[2])
    cross_dot(OWN, 2)
    y_forward(ANT)
    dot_pair(2, ANT, 3)
    z_forward(2, ANT)
    cross_dot(ANT, 0)
    cross_dot(ANT, 1)
    cross_dot(ANT, 2)
    ref_ref[...] = xacc[...].astype(BF)
    dot_pair(2, ANT, 0)
    dot_pair(2, ANT, 1)
    dot_pair(2, ANT, 2)
    layer(3, ref_ref, out_ref, blocks=False)
    drain()


def per_device(
    initial,
    held_cross,
    weights,
    need_rows,
    tiles,
    tile_scale,
    tile_src,
    tile_dst,
    tile_count,
    cross_need,
    cross_tiles,
    cross_scale,
    cross_src,
    cross_dst,
):
    hbm = pl.BlockSpec(memory_space=pl.ANY)
    vmem = pl.BlockSpec(memory_space=pltpu.VMEM)
    smem = pl.BlockSpec(memory_space=pltpu.SMEM)
    dma = pltpu.SemaphoreType.DMA
    table = jax.ShapeDtypeStruct((ROWS, D), BF)
    out = pl.pallas_call(
        kernel,
        out_shape=(table, table),
        in_specs=[hbm, hbm, hbm, vmem, hbm, smem, vmem, vmem, smem, vmem, hbm, smem, vmem, vmem],
        out_specs=(vmem, vmem),
        scratch_shapes=[
            pltpu.VMEM((4, BLOCK, D), BF),
            pltpu.VMEM((ROWS, D), BF),
            pltpu.VMEM((3, D, D), BF),
            pltpu.VMEM((TILES, BLOCK, BLOCK), BF),
            pltpu.VMEM((TILES + 1, BLOCK, BLOCK), F32),
            pltpu.VMEM((SOURCES // 2, ROWS, 2 * BLOCK), BF),
            pltpu.VMEM((XSOURCES // 2, ROWS, 2 * BLOCK), BF),
            pltpu.VMEM((ROWS, D), F32),
            pltpu.VMEM((ROWS, D), F32),
            pltpu.VMEM((ROWS, D), BF),
            pltpu.VMEM((2, 4, BLOCK, D), BF),
            pltpu.VMEM((3, 16, BLOCK, D), BF),
            pltpu.VMEM((4, BLOCK, D), BF),
            pltpu.VMEM((4, BLOCK, D), BF),
            pltpu.VMEM((4, BLOCK, D), BF),
            pltpu.VMEM((2, 2, 2, BLOCK, D), BF),
            pltpu.VMEM((3, 2, 2, BLOCK, D), BF),
            pltpu.VMEM((4, BLOCK, D), BF),
            pltpu.VMEM((2, 7, BLOCK, D), BF),
            pltpu.VMEM((16, BLOCK, D), BF),
            pltpu.VMEM((2, 2, BLOCK, D), BF),
            pltpu.VMEM((2, 6, BLOCK, D), BF),
            pltpu.VMEM((8, BLOCK), I32),
            pltpu.VMEM((8, 8, BLOCK), I32),
            pltpu.VMEM((4, 8, BLOCK), I32),
            pltpu.SMEM((8, 8, BLOCK), I32),
            pltpu.SMEM((4, 8, BLOCK), I32),
            pltpu.VMEM((8, 2 * BLOCK), I32),
            pltpu.VMEM((8, 3 * BLOCK), I32),
            pltpu.SMEM((8, 3 * BLOCK), I32),
            dma((9,)),
            dma((48,)),
            dma((12,)),
            dma((2, 2, 2)),
            dma((3, 4)),
            dma((3, 2, 2)),
            dma((3, 4, 2, 2)),
            dma((4,)),
            dma((2, 2)),
            dma((4, 2)),
        ],
        compiler_params=pltpu.CompilerParams(
            collective_id=0, has_side_effects=True, vmem_limit_bytes=67043328
        ),
    )(
        initial.reshape(4, BLOCK, D),
        held_cross,
        weights,
        need_rows.reshape(1, 16),
        tiles[0, 0],
        tile_scale[0],
        tile_src[0],
        tile_dst[0],
        tile_count,
        cross_need.reshape(1, 16),
        cross_tiles[0, 0],
        cross_scale[0],
        cross_src[0],
        cross_dst[0],
    )
    return out[0], out[1]


def solution(mesh):
    in_specs = (
        P(("comm", "dom"), None),
        P(("comm", "dom"), None),
        P(),
        P("comm", "dom", None, None),
        P("comm", "dom", None, None, None),
        P("comm", "dom", None),
        P("comm", "dom", None),
        P("comm", "dom", None),
        P("comm", "dom"),
        P("comm", "dom", None, None),
        P("comm", "dom", None, None, None),
        P("comm", "dom", None),
        P("comm", "dom", None),
        P("comm", "dom", None),
    )
    out_specs = (P(("comm", "dom"), None), P(("comm", "dom"), None))
    return jax.shard_map(
        per_device, mesh=mesh, in_specs=in_specs, out_specs=out_specs, check_vma=False
    )
```

```python
import functools
import math

import jax
import jax.numpy as jnp
from jax import lax
from jax.experimental import pallas as pl
from jax.experimental.pallas import tpu as pltpu
from jax.sharding import PartitionSpec as P

BLOCK = 128
D = 512
ROWS = 512
TILES = 192
XTILES = 64
SOURCES = 20
XSOURCES = 16
ALPHA = 0.1
LAMBDA = 0.5
MESH = pl.DeviceIdType.MESH
BF = jnp.bfloat16
F32 = jnp.float32
I32 = jnp.int32
OWN, ANT = 0, 1
CA = 384
CB = D - CA
A = pl.ds(0, CA)
B = pl.ds(CA, CB)


def pair(i):
    return pl.ds(i * 2, 2)


def chain_tables(key_ref, tbl_ref, halves, none, row):
    iota0 = lax.broadcasted_iota(I32, (BLOCK, BLOCK), 0)
    iota1 = lax.broadcasted_iota(I32, (BLOCK, BLOCK), 1)
    last = jnp.full((1, BLOCK), -1, I32)
    prev = [jnp.full((1, BLOCK), -1, I32) for _ in range(halves)]
    for h in range(halves):
        down = jnp.broadcast_to(key_ref[0:1, h * BLOCK : (h + 1) * BLOCK], (BLOCK, BLOCK)).T
        who = iota0 + h * BLOCK
        hit = jnp.where(down == iota1, who, -1)
        last = jnp.maximum(last, jnp.max(hit, axis=0, keepdims=True))
        for j in range(h, halves):
            across = jnp.broadcast_to(key_ref[0:1, j * BLOCK : (j + 1) * BLOCK], (BLOCK, BLOCK))
            same = jnp.logical_and(down == across, who < iota1 + j * BLOCK)
            prev[j] = jnp.maximum(prev[j], jnp.max(jnp.where(same, who, -1), axis=0, keepdims=True))
    tbl_ref[row : row + 1, 0:BLOCK] = jnp.where(last < 0, none, last)
    for j in range(halves):
        tbl_ref[row : row + 1, (j + 1) * BLOCK : (j + 2) * BLOCK] = jnp.where(prev[j] < 0, none, prev[j])


def kernel(
    init_hbm,
    held_hbm,
    weights_hbm,
    need_ref,
    tiles_hbm,
    scale_ref,
    src_ref,
    dst_ref,
    count_ref,
    xneed_ref,
    xtiles_hbm,
    xscale_ref,
    xsrc_ref,
    xdst_ref,
    out_ref,
    ref_ref,
    init,
    held,
    weights,
    tiles,
    slots,
    adj,
    xadj,
    acc,
    xacc,
    rounded,
    hbuf,
    rba,
    rbb,
    anta0,
    anta1,
    anta2,
    xfa,
    zfa,
    agm0,
    agm1,
    agm2,
    agp0,
    agp1,
    agp2,
    agz0,
    agz1,
    agz2,
    xfb,
    nba,
    gba,
    gbb,
    cra,
    crb,
    yfa,
    gxa,
    yagm,
    yagp,
    yagz,
    gxb,
    rq,
    reqs,
    xreqs,
    reqs_s,
    xreqs_s,
    keys,
    tbl,
    tbl_s,
    lsem,
    ssem,
    qsem,
    xsa,
    asa,
    zsa,
    rsa,
    ags,
    xsb,
    rsb,
    rpb,
    ns,
    yss,
    csa,
    yags,
    csb,
):
    comm = lax.axis_index("comm")
    dom = lax.axis_index("dom")
    y, xl = comm // 2, comm % 2
    z, xh, c = dom // 4, (dom // 2) % 2, dom % 2
    x = xh * 2 + xl

    def dev(px, py, pz, pc):
        return (py * 2 + px % 2, pz * 4 + (px // 2) * 2 + pc)

    xp, xm, x2 = (x + 1) % 4, (x + 3) % 4, (x + 2) % 4
    xnb = xh * 2 + (1 - xl)
    xot = (x + 3 + 2 * xl) % 4
    zp, zm, z2 = (z + 1) % 4, (z + 3) % 4, (z + 2) % 4
    yp, ym, y2 = (y + 1) % 4, (y + 3) % 4, (y + 2) % 4
    rel_z = (z, zm, zp, z2)
    rel_y = (y, ym, yp, y2)
    anta = (anta0, anta1, anta2)
    agm, agp, agz = (agm0, agm1, agm2), (agp0, agp1, agp2), (agz0, agz1, agz2)
    partner = dev(x, y, z, 1 - c)

    loads = {}

    def load(name, src, dst, i):
        loads[name] = pltpu.make_async_copy(src, dst, lsem.at[i])
        loads[name].start()

    load("init", init_hbm, init, 0)
    load("tiles0", tiles_hbm.at[pl.ds(0, 96)], tiles.at[pl.ds(0, 96)], 1)
    load("tiles1", tiles_hbm.at[pl.ds(96, 96)], tiles.at[pl.ds(96, 96)], 2)
    load("held", held_hbm, held, 3)
    load("weights", weights_hbm, weights, 4)

    barrier = pltpu.get_barrier_semaphore()
    column = [dev(x, y, pz, pc) for pz in (zp, zm, z2) for pc in range(2)]
    across = [dev(x2, y, z, pc) for pc in range(2)]
    peers = [dev(xp, y, z, 0), dev(xp, y, z, 1), dev(xm, y, z, 0), dev(xm, y, z, 1), partner] + column + across
    peers += [dev(x, py, z, c) for py in (yp, ym, y2)]
    for peer in peers:
        pl.semaphore_signal(barrier, inc=1, device_id=peer, device_id_type=MESH)
    rq[0:1, 0:16] = need_ref[...]
    rq[1:3, 0:8] = xneed_ref[...]
    loads["init"].wait()
    pl.semaphore_wait(barrier, len(peers))

    sent = []

    def send(src, dst, sem, device):
        copy = pltpu.make_async_remote_copy(
            src_ref=src,
            dst_ref=dst,
            send_sem=ssem.at[len(sent)],
            recv_sem=sem,
            device_id=device,
            device_id_type=MESH,
        )
        copy.start()
        sent.append(copy)

    def arrived(dst, sem):
        pltpu.make_async_remote_copy(
            src_ref=dst,
            dst_ref=dst,
            send_sem=ssem.at[0],
            recv_sem=sem,
            device_id=partner,
            device_id_type=MESH,
        ).wait_recv()

    def drain():
        for copy in sent:
            copy.wait_send()
        sent.clear()

    def part(pz, ty, pc):
        return pz * 4 + (xh if ty == OWN else 1 - xh) * 2 + pc

    def group(py, ty):
        return py * 2 + (xl if ty == OWN else 1 - xl)


    def xa_first(e, table, half):
        device = dev(xp, y, z, c) if half == 0 else dev(xm, y, z, c)
        for k in range(2):
            send(table.at[2 * half + k, :, A], xfa.at[e, half, k], xsa.at[e, half, k], device)

    def xa_forward(e, k):
        for half in range(2):
            arrived(xfa.at[e, half, k], xsa.at[e, half, k])
            device = dev(xp, y, z, c) if half == 0 else dev(xm, y, z, c)
            send(xfa.at[e, half, k], anta[e].at[2 * half + k], asa.at[e, 2 * half + k], device)

    def xa_done(e):
        for k in range(4):
            arrived(anta[e].at[k], asa.at[e, k])

    def za_gather(ty, table, g, pz, pc, p):
        want = reqs_s[pz * 2 + pc, 0, p]
        gba[ty, g] = table[want, :, A]
        return gba.at[ty, g]

    def za_first(e, ty, table):
        p = part(z, ty, c)
        send(za_gather(ty, table, 0, z2, 0, p), zfa.at[e, 0, ty], zsa.at[e, 0, ty], dev(x, y, zp, c))
        send(za_gather(ty, table, 1, z2, 1, p), zfa.at[e, 1, ty], zsa.at[e, 1, ty], dev(x, y, zm, c))

    def za_rest(e, ty, table):
        p = part(z, ty, c)
        mine = rba.at[e, p]
        send(za_gather(ty, table, 2, zp, 0, p), mine, rsa.at[e, 0, ty, c], dev(x, y, zp, 0))
        send(za_gather(ty, table, 3, zm, 0, p), mine, rsa.at[e, 1, ty, c], dev(x, y, zm, 0))
        send(za_gather(ty, table, 4, zp, 1, p), mine, rsa.at[e, 0, ty, c], dev(x, y, zp, 1))
        send(za_gather(ty, table, 5, zm, 1, p), mine, rsa.at[e, 1, ty, c], dev(x, y, zm, 1))
        send(za_gather(ty, table, 6, z, 1 - c, p), mine, rsa.at[e, 3, ty, 0], partner)
        want = reqs_s[z * 2 + c, 0, p]
        rba[e, p] = table[want, :, A]

    def za_forward(e, ty):
        arrived(zfa.at[e, 0, ty], zsa.at[e, 0, ty])
        send(zfa.at[e, 0, ty], rba.at[e, part(zm, ty, c)], rsa.at[e, 2, ty, c], dev(x, y, zp, 0))
        arrived(zfa.at[e, 1, ty], zsa.at[e, 1, ty])
        send(zfa.at[e, 1, ty], rba.at[e, part(zp, ty, c)], rsa.at[e, 2, ty, c], dev(x, y, zm, 1))


    def ring_first(table, fromm, fromp, sems, up, down):
        low, high = pl.ds(0, 2), pl.ds(2, 2)
        send(table.at[low, :, B], fromm.at[low], sems[0, 0], up)
        send(table.at[high, :, B], fromp.at[high], sems[1, 0], down)
        send(table.at[high, :, B], fromm.at[high], sems[0, 1], up)
        send(table.at[low, :, B], fromp.at[low], sems[1, 1], down)

    def ring_forward(fromm, fromp, far, sems, up, down):
        low, high = pl.ds(0, 2), pl.ds(2, 2)
        arrived(fromm.at[low], sems[0, 0])
        send(fromm.at[low], far.at[low], sems[2, 0], up)
        arrived(fromp.at[high], sems[1, 0])
        send(fromp.at[high], far.at[high], sems[2, 1], down)

    def ring_done(fromm, fromp, sems):
        arrived(fromm.at[pl.ds(2, 2)], sems[0, 1])
        arrived(fromp.at[pl.ds(0, 2)], sems[1, 1])

    def ring_far_done(far, sems):
        arrived(far.at[pl.ds(0, 2)], sems[2, 0])
        arrived(far.at[pl.ds(2, 2)], sems[2, 1])

    def zring(e):
        sems = {(i, j): ags.at[e, i, j] for i in range(3) for j in range(2)}
        return agm[e], agp[e], agz[e], sems, dev(x, y, zp, c), dev(x, y, zm, c)

    def zb_first(e, table):
        m, p, _, sems, up, down = zring(e)
        ring_first(table, m, p, sems, up, down)

    def zb_forward(e):
        ring_forward(*zring(e))

    def zb_done(e):
        m, p, _, sems, _, _ = zring(e)
        ring_done(m, p, sems)

    def zb_far_done(e):
        _, _, far, sems, _, _ = zring(e)
        ring_far_done(far, sems)

    def xb_first(e, r, own=None):
        table = (own, agm[e], agp[e], agz[e])[r]
        p = part(rel_z[r], OWN, c)

        def wanted(row):
            want = reqs_s[row, 0, p]
            return table[want, :, B] if r == 0 else table[want]

        gbb[3 * r] = wanted(8)
        send(gbb.at[3 * r], xfb.at[e, 0, r], xsb.at[e, 0, r], dev(xp, y, z, c))
        gbb[3 * r + 1] = wanted(9)
        send(gbb.at[3 * r + 1], xfb.at[e, 1, r], xsb.at[e, 1, r], dev(xm, y, z, c))
        gbb[3 * r + 2] = wanted(z * 2 + 1 - c)
        send(gbb.at[3 * r + 2], rbb.at[e, p], rpb.at[e, r], partner)
        rbb[e, p] = wanted(z * 2 + c)

    def xb_forward(e, r):
        arrived(xfb.at[e, 0, r], xsb.at[e, 0, r])
        send(xfb.at[e, 0, r], rbb.at[e, rel_z[r] * 4 + (xm // 2) * 2 + c], rsb.at[e, r, c], dev(xp, y, z, 0))
        arrived(xfb.at[e, 1, r], xsb.at[e, 1, r])
        send(xfb.at[e, 1, r], rbb.at[e, rel_z[r] * 4 + (xp // 2) * 2 + c], rsb.at[e, r, c], dev(xm, y, z, 1))


    def dot_into(total, lhs, rhs, start, width, first=False):
        for n in range(0, width, 256):
            w = min(256, width - n)
            cols = pl.ds(start + n, w)
            value = jnp.dot(lhs[...], rhs[:, :, n : n + w].reshape(256, w), preferred_element_type=F32)
            if first:
                total[:, cols] = value
            else:
                total[:, cols] += value

    def dot_own(table):
        dot_into(acc, adj.at[0], table.at[pl.ds(0, 2)], 0, D, first=True)
        dot_into(acc, adj.at[1], table.at[pl.ds(2, 2)], 0, D)

    def dot_a(e, ty, key):
        pz = (zm, zp, z2, z)[key]
        if key == 3:
            arrived(rba.at[e, part(z, ty, 1 - c)], rsa.at[e, 3, ty, 0])
        else:
            for pc in range(2):
                arrived(rba.at[e, part(pz, ty, pc)], rsa.at[e, key, ty, pc])
        j = pz * 2 + (xh if ty == OWN else 1 - xh)
        dot_into(acc, adj.at[2 + j], rba.at[e, pair(j)], 0, CA)

    def dot_b(e, ty, r):
        if ty == OWN:
            arrived(rbb.at[e, part(rel_z[r], OWN, 1 - c)], rpb.at[e, r])
        else:
            for pc in range(2):
                arrived(rbb.at[e, part(rel_z[r], ANT, pc)], rsb.at[e, r, pc])
        j = rel_z[r] * 2 + (xh if ty == OWN else 1 - xh)
        dot_into(acc, adj.at[2 + j], rbb.at[e, pair(j)], CA, CB)

    def layer(level, added, target, after=lambda half: None, blocks=True):
        beta = math.log(LAMBDA / level + 1.0)
        for half in range(2):
            rows = pl.ds(half * 256, 256)
            total = acc[rows, :] + added[rows, :].astype(F32)
            mixed = (1.0 - ALPHA) * total + ALPHA * init[2 * half : 2 * half + 2].reshape(256, D).astype(F32)
            acc[rows, :] = mixed
            rounded[rows, :] = mixed.astype(BF)
            for n in range(2):
                cols = pl.ds(n * 256, 256)
                turned = jnp.dot(rounded[rows, :], weights[level - 1, :, cols], preferred_element_type=F32)
                done = jax.nn.relu((1.0 - beta) * acc[rows, cols] + beta * turned).astype(BF)
                if blocks:
                    target[2 * half : 2 * half + 2, :, cols] = done.reshape(2, BLOCK, 256)
                else:
                    target[rows, cols] = done
            after(half)


    def chain(tile_ref, scales, row, start, stop):
        @pl.loop(start, stop)
        def _(t):
            before = tbl_s[row, BLOCK + t]
            slots[t] = slots[before] + scales[0, t] * tile_ref[t].astype(F32)

    def place(target, row, sources):
        @pl.loop(0, sources // 2)
        def _(s2):
            for b in range(4):
                for s in range(2):
                    final = tbl_s[row, b * sources + s2 * 2 + s]
                    target[s2, b * BLOCK : (b + 1) * BLOCK, s * BLOCK : (s + 1) * BLOCK] = slots[final].astype(BF)

    for device in column + [partner]:
        send(rq, reqs.at[z * 2 + c], qsem.at[z * 2 + c], device)
    for device in across:
        send(rq, reqs.at[8 + c], qsem.at[8 + c], device)
    for py in (yp, ym, y2):
        send(rq, xreqs.at[y], qsem.at[10 + y], dev(x, py, z, c))
    send(rq, xreqs.at[4], qsem.at[14], dev(xnb, y, z, c))
    xa_first(0, init, 0)
    xa_first(0, init, 1)
    zb_first(0, init)
    reqs[z * 2 + c] = rq[...]
    xreqs[y] = rq[...]

    keys[...] = jnp.full((8, 256), -1, I32)
    live = count_ref[0, 0]
    at = lax.broadcasted_iota(I32, (1, TILES), 1)
    keys[0:1, 0:TILES] = jnp.where(at < live, dst_ref[...] * SOURCES + src_ref[...], -1)
    chain_tables(keys, tbl, 2, TILES, 0)
    keys[0:1, 0:256] = jnp.full((1, 256), -1, I32)
    keys[0:1, 0:XTILES] = xdst_ref[...] * XSOURCES + xsrc_ref[...]
    chain_tables(keys, tbl, 1, TILES, 1)
    copy_tbl = pltpu.make_async_copy(tbl, tbl_s, lsem.at[5])
    copy_tbl.start()
    slots[TILES] = jnp.zeros((BLOCK, BLOCK), F32)

    for pz in (zp, zm, z2):
        for pc in range(2):
            arrived(reqs.at[pz * 2 + pc], qsem.at[pz * 2 + pc])
    arrived(reqs.at[z * 2 + 1 - c], qsem.at[z * 2 + 1 - c])
    for pc in range(2):
        arrived(reqs.at[8 + pc], qsem.at[8 + pc])
    copy_req = pltpu.make_async_copy(reqs, reqs_s, lsem.at[6])
    copy_req.start()
    copy_req.wait()

    def begin(e, table):
        za_first(e, OWN, table)
        xb_first(e, 0, table)

    begin(0, init)
    zb_forward(0)
    za_rest(0, OWN, init)
    for py in (yp, ym, y2):
        arrived(xreqs.at[py], qsem.at[10 + py])
    arrived(xreqs.at[4], qsem.at[14])
    copy_xreq = pltpu.make_async_copy(xreqs, xreqs_s, lsem.at[7])
    copy_xreq.start()
    copy_xreq.wait()
    copy_tbl.wait()
    loads["tiles0"].wait()
    xa_forward(0, 0)
    zb_done(0)
    xb_first(0, 1)
    xb_first(0, 2)
    chain(tiles, scale_ref, 0, 0, 32)
    xa_forward(0, 1)
    chain(tiles, scale_ref, 0, 32, 64)
    za_forward(0, OWN)
    xb_forward(0, 0)
    zb_far_done(0)
    xb_first(0, 3)
    chain(tiles, scale_ref, 0, 64, 96)
    loads["tiles1"].wait()
    xb_forward(0, 1)
    xb_forward(0, 2)
    chain(tiles, scale_ref, 0, 96, 144)
    xa_done(0)
    za_first(0, ANT, anta[0])
    za_rest(0, ANT, anta[0])
    xb_forward(0, 3)
    chain(tiles, scale_ref, 0, 144, 192)
    load("xtiles", xtiles_hbm, tiles.at[pl.ds(0, XTILES)], 8)
    place(adj, 0, SOURCES)
    dot_own(init)
    za_forward(0, ANT)
    for key in (3, 0, 1, 2):
        dot_a(0, OWN, key)
    for r in range(4):
        dot_b(0, OWN, r)
        dot_b(0, ANT, r)
    loads["held"].wait()
    loads["weights"].wait()
    for key in (3, 0, 1, 2):
        dot_a(0, ANT, key)
    drain()
    layer(1, held, hbuf.at[0], lambda half: xa_first(1, hbuf.at[0], half))

    h1 = hbuf.at[0]
    zb_first(1, h1)
    begin(1, h1)
    dot_own(h1)
    zb_forward(1)
    za_rest(1, OWN, h1)
    xa_forward(1, 0)
    zb_done(1)
    xb_first(1, 1)
    xb_first(1, 2)
    dot_a(1, OWN, 3)
    dot_b(1, OWN, 0)
    xa_forward(1, 1)
    xb_forward(1, 0)
    za_forward(1, OWN)
    zb_far_done(1)
    xb_first(1, 3)
    dot_b(1, OWN, 1)
    dot_b(1, OWN, 2)
    dot_b(1, OWN, 3)
    xb_forward(1, 1)
    xb_forward(1, 2)
    xa_done(1)
    za_first(1, ANT, anta[1])
    za_rest(1, ANT, anta[1])
    xb_forward(1, 3)
    dot_a(1, OWN, 0)
    dot_a(1, OWN, 1)
    dot_a(1, OWN, 2)
    dot_a(1, ANT, 3)
    dot_b(1, ANT, 0)
    za_forward(1, ANT)
    loads["xtiles"].wait()
    chain(tiles, xscale_ref, 1, 0, XTILES)
    place(xadj, 1, XSOURCES)
    for r in range(1, 4):
        dot_b(1, ANT, r)
    for key in (0, 1, 2):
        dot_a(1, ANT, key)
    drain()

    h2 = hbuf.at[1]

    def na_first(half):
        for k in range(2 * half, 2 * half + 2):
            send(h2.at[k, :, A], nba.at[k], ns.at[k], dev(xnb, y, z, c))

    def na_forward(k):
        arrived(nba.at[k], ns.at[k])
        send(nba.at[k], anta[2].at[k], asa.at[2, k], dev(xot, y, z, c))

    def ya_gather(ty, table, g, py, k):
        want = xreqs_s[py, 1 + k, group(y, ty)]
        gxa[ty, g] = table[want, :, A]

    def ya_first(ty, table):
        ya_gather(ty, table, 0, y2, 0)
        send(gxa.at[ty, 0], yfa.at[0, ty], yss.at[0, ty], dev(x, yp, z, c))
        ya_gather(ty, table, 1, y2, 1)
        send(gxa.at[ty, 1], yfa.at[1, ty], yss.at[1, ty], dev(x, ym, z, c))

    def ya_rest(ty, table):
        mine = cra.at[pair(group(y, ty))]
        for i, py in enumerate((yp, ym)):
            ya_gather(ty, table, 2 + 2 * i, py, 0)
            ya_gather(ty, table, 3 + 2 * i, py, 1)
            send(gxa.at[ty, pair(1 + i)], mine, csa.at[i, ty], dev(x, py, z, c))
        for k in range(2):
            want = xreqs_s[y, 1 + k, group(y, ty)]
            cra[group(y, ty) * 2 + k] = table[want, :, A]

    def ya_forward(ty):
        arrived(yfa.at[0, ty], yss.at[0, ty])
        send(yfa.at[0, ty], cra.at[group(ym, ty) * 2], csa.at[2, ty], dev(x, yp, z, c))
        arrived(yfa.at[1, ty], yss.at[1, ty])
        send(yfa.at[1, ty], cra.at[group(yp, ty) * 2 + 1], csa.at[3, ty], dev(x, ym, z, c))

    ysems = {(i, j): yags.at[i, j] for i in range(3) for j in range(2)}
    yring = (yagm, yagp, yagz, ysems, dev(x, yp, z, c), dev(x, ym, z, c))

    def yb_first(r):
        table = (h2, yagm, yagp, yagz)[r]
        g = group(rel_y[r], OWN)
        for k in range(2):
            for row, keep in ((4, False), (y, True)):
                want = xreqs_s[row, 1 + k, g]
                value = table[want, :, B] if r == 0 else table[want]
                if keep:
                    crb[g * 2 + k] = value
                else:
                    gxb[2 * r + k] = value
        send(gxb.at[pl.ds(2 * r, 2)], crb.at[pair(g)], csb.at[r], dev(xnb, y, z, c))

    def cross_a(ty, key, first=False):
        py = (ym, yp, y2, y)[key]
        g = group(py, ty)
        if key < 2:
            arrived(cra.at[pair(g)], csa.at[key, ty])
        if key == 2:
            arrived(cra.at[g * 2], csa.at[2, ty])
            arrived(cra.at[g * 2 + 1], csa.at[3, ty])
        dot_into(xacc, xadj.at[g], cra.at[pair(g)], 0, CA, first)

    def cross_b(ty, r, first=False):
        g = group(rel_y[r], ty)
        if ty == ANT:
            arrived(crb.at[pair(g)], csb.at[r])
        dot_into(xacc, xadj.at[g], crb.at[pair(g)], CA, CB, first)

    layer(2, held, h2, na_first)
    zb_first(2, h2)
    ring_first(h2, yagm, yagp, ysems, dev(x, yp, z, c), dev(x, ym, z, c))
    za_first(2, OWN, h2)
    ya_first(OWN, h2)
    xb_first(2, 0, h2)
    zb_forward(2)
    ring_forward(*yring)
    za_rest(2, OWN, h2)
    ya_rest(OWN, h2)
    na_forward(0)
    zb_done(2)
    xb_first(2, 1)
    xb_first(2, 2)
    yb_first(0)
    na_forward(1)
    ring_done(yagm, yagp, ysems)
    yb_first(1)
    yb_first(2)
    dot_own(h2)
    na_forward(2)
    za_forward(2, OWN)
    ya_forward(OWN)
    zb_far_done(2)
    xb_first(2, 3)
    ring_far_done(yagz, ysems)
    yb_first(3)
    na_forward(3)
    ya_first(ANT, nba)
    ya_rest(ANT, nba)
    xb_forward(2, 0)
    cross_a(OWN, 3, first=True)
    cross_a(ANT, 3)
    cross_b(OWN, 0, first=True)
    xb_forward(2, 1)
    xb_forward(2, 2)
    xa_done(2)
    za_first(2, ANT, anta[2])
    za_rest(2, ANT, anta[2])
    xb_forward(2, 3)
    for key in (3, 0, 1):
        dot_a(2, OWN, key)
    cross_a(OWN, 0)
    cross_a(OWN, 1)
    ya_forward(ANT)
    za_forward(2, ANT)
    for r in range(1, 4):
        cross_b(OWN, r)
    dot_a(2, OWN, 2)
    cross_a(OWN, 2)
    for r in range(4):
        dot_b(2, OWN, r)
    dot_a(2, ANT, 3)
    for r in range(4):
        dot_b(2, ANT, r)
        cross_b(ANT, r)
    cross_a(ANT, 0)
    cross_a(ANT, 1)
    dot_a(2, ANT, 0)
    dot_a(2, ANT, 1)
    cross_a(ANT, 2)
    ref_ref[...] = xacc[...].astype(BF)
    dot_a(2, ANT, 2)
    layer(3, ref_ref, out_ref, blocks=False)
    drain()


def per_device(
    initial,
    held_cross,
    weights,
    need_rows,
    tiles,
    tile_scale,
    tile_src,
    tile_dst,
    tile_count,
    cross_need,
    cross_tiles,
    cross_scale,
    cross_src,
    cross_dst,
):
    hbm = pl.BlockSpec(memory_space=pl.ANY)
    vmem = pl.BlockSpec(memory_space=pltpu.VMEM)
    smem = pl.BlockSpec(memory_space=pltpu.SMEM)
    dma = pltpu.SemaphoreType.DMA
    table = jax.ShapeDtypeStruct((ROWS, D), BF)
    out = pl.pallas_call(
        kernel,
        out_shape=(table, table),
        in_specs=[hbm, hbm, hbm, vmem, hbm, smem, vmem, vmem, smem, vmem, hbm, smem, vmem, vmem],
        out_specs=(vmem, vmem),
        scratch_shapes=[
            pltpu.VMEM((4, BLOCK, D), BF),
            pltpu.VMEM((ROWS, D), BF),
            pltpu.VMEM((3, D, D), BF),
            pltpu.VMEM((TILES, BLOCK, BLOCK), BF),
            pltpu.VMEM((TILES + 1, BLOCK, BLOCK), F32),
            pltpu.VMEM((SOURCES // 2, ROWS, 2 * BLOCK), BF),
            pltpu.VMEM((XSOURCES // 2, ROWS, 2 * BLOCK), BF),
            pltpu.VMEM((ROWS, D), F32),
            pltpu.VMEM((ROWS, D), F32),
            pltpu.VMEM((ROWS, D), BF),
            pltpu.VMEM((2, 4, BLOCK, D), BF),
            pltpu.VMEM((3, 16, BLOCK, CA), BF),
            pltpu.VMEM((3, 16, BLOCK, CB), BF),
            pltpu.VMEM((4, BLOCK, CA), BF),
            pltpu.VMEM((4, BLOCK, CA), BF),
            pltpu.VMEM((4, BLOCK, CA), BF),
            pltpu.VMEM((2, 2, 2, BLOCK, CA), BF),
            pltpu.VMEM((3, 2, 2, BLOCK, CA), BF),
            pltpu.VMEM((4, BLOCK, CB), BF),
            pltpu.VMEM((4, BLOCK, CB), BF),
            pltpu.VMEM((4, BLOCK, CB), BF),
            pltpu.VMEM((4, BLOCK, CB), BF),
            pltpu.VMEM((4, BLOCK, CB), BF),
            pltpu.VMEM((4, BLOCK, CB), BF),
            pltpu.VMEM((4, BLOCK, CB), BF),
            pltpu.VMEM((4, BLOCK, CB), BF),
            pltpu.VMEM((4, BLOCK, CB), BF),
            pltpu.VMEM((3, 2, 4, BLOCK, CB), BF),
            pltpu.VMEM((4, BLOCK, CA), BF),
            pltpu.VMEM((2, 7, BLOCK, CA), BF),
            pltpu.VMEM((12, BLOCK, CB), BF),
            pltpu.VMEM((16, BLOCK, CA), BF),
            pltpu.VMEM((16, BLOCK, CB), BF),
            pltpu.VMEM((2, 2, BLOCK, CA), BF),
            pltpu.VMEM((2, 6, BLOCK, CA), BF),
            pltpu.VMEM((4, BLOCK, CB), BF),
            pltpu.VMEM((4, BLOCK, CB), BF),
            pltpu.VMEM((4, BLOCK, CB), BF),
            pltpu.VMEM((8, BLOCK, CB), BF),
            pltpu.VMEM((4, BLOCK), I32),
            pltpu.VMEM((10, 4, BLOCK), I32),
            pltpu.VMEM((5, 4, BLOCK), I32),
            pltpu.SMEM((10, 4, BLOCK), I32),
            pltpu.SMEM((5, 4, BLOCK), I32),
            pltpu.VMEM((8, 2 * BLOCK), I32),
            pltpu.VMEM((8, 3 * BLOCK), I32),
            pltpu.SMEM((8, 3 * BLOCK), I32),
            dma((9,)),
            dma((96,)),
            dma((15,)),
            dma((2, 2, 2)),
            dma((3, 4)),
            dma((3, 2, 2)),
            dma((3, 4, 2, 2)),
            dma((3, 3, 2)),
            dma((3, 2, 4)),
            dma((3, 4, 2)),
            dma((3, 4)),
            dma((4,)),
            dma((2, 2)),
            dma((4, 2)),
            dma((3, 2)),
            dma((4,)),
        ],
        compiler_params=pltpu.CompilerParams(
            collective_id=0, has_side_effects=True, vmem_limit_bytes=67043328
        ),
    )(
        initial.reshape(4, BLOCK, D),
        held_cross,
        weights,
        need_rows.reshape(1, 16),
        tiles[0, 0],
        tile_scale[0],
        tile_src[0],
        tile_dst[0],
        tile_count,
        cross_need[0, 0].T,
        cross_tiles[0, 0],
        cross_scale[0],
        cross_src[0],
        cross_dst[0],
    )
    return out[0], out[1]


def solution(mesh):
    in_specs = (
        P(("comm", "dom"), None),
        P(("comm", "dom"), None),
        P(),
        P("comm", "dom", None, None),
        P("comm", "dom", None, None, None),
        P("comm", "dom", None),
        P("comm", "dom", None),
        P("comm", "dom", None),
        P("comm", "dom"),
        P("comm", "dom", None, None),
        P("comm", "dom", None, None, None),
        P("comm", "dom", None),
        P("comm", "dom", None),
        P("comm", "dom", None),
    )
    out_specs = (P(("comm", "dom"), None), P(("comm", "dom"), None))
    return jax.shard_map(
        per_device, mesh=mesh, in_specs=in_specs, out_specs=out_specs, check_vma=False
    )
```

```python
import functools
import math

import jax
import jax.numpy as jnp
from jax import lax
from jax.experimental import pallas as pl
from jax.experimental.pallas import tpu as pltpu
from jax.sharding import PartitionSpec as P

BLOCK = 128
D = 512
ROWS = 512
TILES = 192
XTILES = 64
SOURCES = 20
XSOURCES = 16
ALPHA = 0.1
LAMBDA = 0.5
MESH = pl.DeviceIdType.MESH
BF = jnp.bfloat16
F32 = jnp.float32
I32 = jnp.int32
OWN, ANT = 0, 1
CA = (256, 256, 384)
CB = tuple(D - n for n in CA)


def pair(i):
    return pl.ds(i * 2, 2)


def chain_tables(key_ref, tbl_ref, halves, none, row):
    iota0 = lax.broadcasted_iota(I32, (BLOCK, BLOCK), 0)
    iota1 = lax.broadcasted_iota(I32, (BLOCK, BLOCK), 1)
    last = jnp.full((1, BLOCK), -1, I32)
    prev = [jnp.full((1, BLOCK), -1, I32) for _ in range(halves)]
    for h in range(halves):
        down = jnp.broadcast_to(key_ref[0:1, h * BLOCK : (h + 1) * BLOCK], (BLOCK, BLOCK)).T
        who = iota0 + h * BLOCK
        hit = jnp.where(down == iota1, who, -1)
        last = jnp.maximum(last, jnp.max(hit, axis=0, keepdims=True))
        for j in range(h, halves):
            across = jnp.broadcast_to(key_ref[0:1, j * BLOCK : (j + 1) * BLOCK], (BLOCK, BLOCK))
            same = jnp.logical_and(down == across, who < iota1 + j * BLOCK)
            prev[j] = jnp.maximum(prev[j], jnp.max(jnp.where(same, who, -1), axis=0, keepdims=True))
    tbl_ref[row : row + 1, 0:BLOCK] = jnp.where(last < 0, none, last)
    for j in range(halves):
        tbl_ref[row : row + 1, (j + 1) * BLOCK : (j + 2) * BLOCK] = jnp.where(prev[j] < 0, none, prev[j])


def kernel(
    init_hbm,
    held_hbm,
    weights_hbm,
    need_ref,
    tiles_hbm,
    scale_ref,
    src_ref,
    dst_ref,
    count_ref,
    xneed_ref,
    xtiles_hbm,
    xscale_ref,
    xsrc_ref,
    xdst_ref,
    out_ref,
    ref_ref,
    init,
    held,
    weights,
    tiles,
    slots,
    adj,
    xadj,
    acc,
    xacc,
    rounded,
    hbuf,
    rba0,
    rba1,
    rba2,
    rbb0,
    rbb1,
    rbb2,
    anta0,
    anta1,
    anta2,
    xfa,
    zfa0,
    zfa1,
    zfa2,
    agm0,
    agm1,
    agm2,
    agp0,
    agp1,
    agp2,
    agz0,
    agz1,
    agz2,
    xfb0,
    xfb1,
    xfb2,
    nba,
    xfo,
    gba0,
    gba2,
    gbb0,
    gbb2,
    cra,
    crb,
    yfa,
    gxa,
    yagm,
    yagp,
    yagz,
    gxb,
    rq,
    reqs,
    xreqs,
    reqs_s,
    xreqs_s,
    keys,
    tbl,
    tbl_s,
    lsem,
    ssem,
    qsem,
    xsa,
    asa,
    zsa,
    rsa,
    ags,
    xsb,
    rsb,
    rpb,
    ns,
    os,
    yss,
    csa,
    yags,
    csb,
):
    comm = lax.axis_index("comm")
    dom = lax.axis_index("dom")
    y, xl = comm // 2, comm % 2
    z, xh, c = dom // 4, (dom // 2) % 2, dom % 2
    x = xh * 2 + xl

    def dev(px, py, pz, pc):
        return (py * 2 + px % 2, pz * 4 + (px // 2) * 2 + pc)

    xp, xm, x2 = (x + 1) % 4, (x + 3) % 4, (x + 2) % 4
    xnb = xh * 2 + (1 - xl)
    xot = (x + 3 + 2 * xl) % 4
    zp, zm, z2 = (z + 1) % 4, (z + 3) % 4, (z + 2) % 4
    yp, ym, y2 = (y + 1) % 4, (y + 3) % 4, (y + 2) % 4
    rel_z = (z, zm, zp, z2)
    rel_y = (y, ym, yp, y2)
    anta = (anta0, anta1, anta2)
    agm, agp, agz = (agm0, agm1, agm2), (agp0, agp1, agp2), (agz0, agz1, agz2)
    partner = dev(x, y, z, 1 - c)

    rba, rbb = (rba0, rba1, rba2), (rbb0, rbb1, rbb2)
    zfa, xfb = (zfa0, zfa1, zfa2), (xfb0, xfb1, xfb2)
    gba, gbb = (gba0, gba0, gba2), (gbb0, gbb0, gbb2)
    cols_a = tuple(pl.ds(0, n) for n in CA)
    cols_b = tuple(pl.ds(n, D - n) for n in CA)

    loads = {}

    def load(name, src, dst, i):
        loads[name] = pltpu.make_async_copy(src, dst, lsem.at[i])
        loads[name].start()

    load("init", init_hbm, init, 0)
    load("tiles0", tiles_hbm.at[pl.ds(0, 96)], tiles.at[pl.ds(0, 96)], 1)
    load("tiles1", tiles_hbm.at[pl.ds(96, 96)], tiles.at[pl.ds(96, 96)], 2)
    load("held", held_hbm, held, 3)
    load("weights", weights_hbm, weights, 4)

    barrier = pltpu.get_barrier_semaphore()
    column = [dev(x, y, pz, pc) for pz in (zp, zm, z2) for pc in range(2)]
    across = [dev(x2, y, z, pc) for pc in range(2)]
    peers = [dev(xp, y, z, 0), dev(xp, y, z, 1), dev(xm, y, z, 0), dev(xm, y, z, 1), partner] + column + across
    peers += [dev(x, py, z, c) for py in (yp, ym, y2)]
    for peer in peers:
        pl.semaphore_signal(barrier, inc=1, device_id=peer, device_id_type=MESH)
    rq[0:1, 0:16] = need_ref[...]
    rq[1:3, 0:8] = xneed_ref[...]
    loads["init"].wait()
    pl.semaphore_wait(barrier, len(peers))

    sent = []

    def send(src, dst, sem, device):
        copy = pltpu.make_async_remote_copy(
            src_ref=src,
            dst_ref=dst,
            send_sem=ssem.at[len(sent)],
            recv_sem=sem,
            device_id=device,
            device_id_type=MESH,
        )
        copy.start()
        sent.append(copy)

    def arrived(dst, sem):
        pltpu.make_async_remote_copy(
            src_ref=dst,
            dst_ref=dst,
            send_sem=ssem.at[0],
            recv_sem=sem,
            device_id=partner,
            device_id_type=MESH,
        ).wait_recv()

    def drain():
        for copy in sent:
            copy.wait_send()
        sent.clear()

    def part(pz, ty, pc):
        return pz * 4 + (xh if ty == OWN else 1 - xh) * 2 + pc

    def group(py, ty):
        return py * 2 + (xl if ty == OWN else 1 - xl)


    def xa_first(e, table, half):
        device = dev(xp, y, z, c) if half == 0 else dev(xm, y, z, c)
        for k in range(2):
            send(table.at[2 * half + k, :, cols_a[e]], xfa.at[e, half, k], xsa.at[e, half, k], device)

    def xa_forward(e, k):
        for half in range(2):
            arrived(xfa.at[e, half, k], xsa.at[e, half, k])
            device = dev(xp, y, z, c) if half == 0 else dev(xm, y, z, c)
            send(xfa.at[e, half, k], anta[e].at[2 * half + k], asa.at[e, 2 * half + k], device)

    def xa_done(e):
        for k in range(4):
            arrived(anta[e].at[k], asa.at[e, k])

    def za_gather(e, ty, table, g, pz, pc, p):
        want = reqs_s[pz * 2 + pc, 0, p]
        gba[e][ty, g] = table[want, :, cols_a[e]]
        return gba[e].at[ty, g]

    def za_first(e, ty, table):
        p = part(z, ty, c)
        send(za_gather(e, ty, table, 0, z2, 0, p), zfa[e].at[0, ty], zsa.at[e, 0, ty], dev(x, y, zp, c))
        send(za_gather(e, ty, table, 1, z2, 1, p), zfa[e].at[1, ty], zsa.at[e, 1, ty], dev(x, y, zm, c))

    def za_rest(e, ty, table):
        p = part(z, ty, c)
        mine = rba[e].at[p]
        send(za_gather(e, ty, table, 2, zp, 0, p), mine, rsa.at[e, 0, ty, c], dev(x, y, zp, 0))
        send(za_gather(e, ty, table, 3, zm, 0, p), mine, rsa.at[e, 1, ty, c], dev(x, y, zm, 0))
        send(za_gather(e, ty, table, 4, zp, 1, p), mine, rsa.at[e, 0, ty, c], dev(x, y, zp, 1))
        send(za_gather(e, ty, table, 5, zm, 1, p), mine, rsa.at[e, 1, ty, c], dev(x, y, zm, 1))
        send(za_gather(e, ty, table, 6, z, 1 - c, p), mine, rsa.at[e, 3, ty, 0], partner)
        want = reqs_s[z * 2 + c, 0, p]
        rba[e][p] = table[want, :, cols_a[e]]

    def za_forward(e, ty):
        arrived(zfa[e].at[0, ty], zsa.at[e, 0, ty])
        send(zfa[e].at[0, ty], rba[e].at[part(zm, ty, c)], rsa.at[e, 2, ty, c], dev(x, y, zp, 0))
        arrived(zfa[e].at[1, ty], zsa.at[e, 1, ty])
        send(zfa[e].at[1, ty], rba[e].at[part(zp, ty, c)], rsa.at[e, 2, ty, c], dev(x, y, zm, 1))


    def ring_first(table, b, fromm, fromp, sems, up, down):
        low, high = pl.ds(0, 2), pl.ds(2, 2)
        send(table.at[low, :, b], fromm.at[low], sems[0, 0], up)
        send(table.at[high, :, b], fromp.at[high], sems[1, 0], down)
        send(table.at[high, :, b], fromm.at[high], sems[0, 1], up)
        send(table.at[low, :, b], fromp.at[low], sems[1, 1], down)

    def ring_forward(fromm, fromp, far, sems, up, down):
        low, high = pl.ds(0, 2), pl.ds(2, 2)
        arrived(fromm.at[low], sems[0, 0])
        send(fromm.at[low], far.at[low], sems[2, 0], up)
        arrived(fromp.at[high], sems[1, 0])
        send(fromp.at[high], far.at[high], sems[2, 1], down)

    def ring_done(fromm, fromp, sems):
        arrived(fromm.at[pl.ds(2, 2)], sems[0, 1])
        arrived(fromp.at[pl.ds(0, 2)], sems[1, 1])

    def ring_far_done(far, sems):
        arrived(far.at[pl.ds(0, 2)], sems[2, 0])
        arrived(far.at[pl.ds(2, 2)], sems[2, 1])

    def zring(e):
        sems = {(i, j): ags.at[e, i, j] for i in range(3) for j in range(2)}
        return agm[e], agp[e], agz[e], sems, dev(x, y, zp, c), dev(x, y, zm, c)

    def zb_first(e, table):
        m, p, _, sems, up, down = zring(e)
        ring_first(table, cols_b[e], m, p, sems, up, down)

    def zb_forward(e):
        ring_forward(*zring(e))

    def zb_done(e):
        m, p, _, sems, _, _ = zring(e)
        ring_done(m, p, sems)

    def zb_far_done(e):
        _, _, far, sems, _, _ = zring(e)
        ring_far_done(far, sems)

    def xb_first(e, r, own=None):
        table = (own, agm[e], agp[e], agz[e])[r]
        p = part(rel_z[r], OWN, c)

        def wanted(row):
            want = reqs_s[row, 0, p]
            return table[want, :, cols_b[e]] if r == 0 else table[want]

        gbb[e][3 * r] = wanted(8)
        send(gbb[e].at[3 * r], xfb[e].at[0, r], xsb.at[e, 0, r], dev(xp, y, z, c))
        gbb[e][3 * r + 1] = wanted(9)
        send(gbb[e].at[3 * r + 1], xfb[e].at[1, r], xsb.at[e, 1, r], dev(xm, y, z, c))
        gbb[e][3 * r + 2] = wanted(z * 2 + 1 - c)
        send(gbb[e].at[3 * r + 2], rbb[e].at[p], rpb.at[e, r], partner)
        rbb[e][p] = wanted(z * 2 + c)

    def xb_forward(e, r):
        arrived(xfb[e].at[0, r], xsb.at[e, 0, r])
        send(xfb[e].at[0, r], rbb[e].at[rel_z[r] * 4 + (xm // 2) * 2 + c], rsb.at[e, r, c], dev(xp, y, z, 0))
        arrived(xfb[e].at[1, r], xsb.at[e, 1, r])
        send(xfb[e].at[1, r], rbb[e].at[rel_z[r] * 4 + (xp // 2) * 2 + c], rsb.at[e, r, c], dev(xm, y, z, 1))


    def dot_into(total, lhs, rhs, start, width, first=False):
        for n in range(0, width, 256):
            w = min(256, width - n)
            cols = pl.ds(start + n, w)
            value = jnp.dot(lhs[...], rhs[:, :, n : n + w].reshape(256, w), preferred_element_type=F32)
            if first:
                total[:, cols] = value
            else:
                total[:, cols] += value

    def dot_own(table):
        dot_into(acc, adj.at[0], table.at[pl.ds(0, 2)], 0, D, first=True)
        dot_into(acc, adj.at[1], table.at[pl.ds(2, 2)], 0, D)

    def dot_a(e, ty, key):
        pz = (zm, zp, z2, z)[key]
        if key == 3:
            arrived(rba[e].at[part(z, ty, 1 - c)], rsa.at[e, 3, ty, 0])
        else:
            for pc in range(2):
                arrived(rba[e].at[part(pz, ty, pc)], rsa.at[e, key, ty, pc])
        j = pz * 2 + (xh if ty == OWN else 1 - xh)
        dot_into(acc, adj.at[2 + j], rba[e].at[pair(j)], 0, CA[e])

    def dot_b(e, ty, r):
        if ty == OWN:
            arrived(rbb[e].at[part(rel_z[r], OWN, 1 - c)], rpb.at[e, r])
        else:
            for pc in range(2):
                arrived(rbb[e].at[part(rel_z[r], ANT, pc)], rsb.at[e, r, pc])
        j = rel_z[r] * 2 + (xh if ty == OWN else 1 - xh)
        dot_into(acc, adj.at[2 + j], rbb[e].at[pair(j)], CA[e], CB[e])

    def layer(level, added, target, after=lambda half: None, blocks=True):
        beta = math.log(LAMBDA / level + 1.0)
        for half in range(2):
            rows = pl.ds(half * 256, 256)
            total = acc[rows, :] + added[rows, :].astype(F32)
            mixed = (1.0 - ALPHA) * total + ALPHA * init[2 * half : 2 * half + 2].reshape(256, D).astype(F32)
            acc[rows, :] = mixed
            rounded[rows, :] = mixed.astype(BF)
            for n in range(2):
                cols = pl.ds(n * 256, 256)
                turned = jnp.dot(rounded[rows, :], weights[level - 1, :, cols], preferred_element_type=F32)
                done = jax.nn.relu((1.0 - beta) * acc[rows, cols] + beta * turned).astype(BF)
                if blocks:
                    target[2 * half : 2 * half + 2, :, cols] = done.reshape(2, BLOCK, 256)
                else:
                    target[rows, cols] = done
            after(half)


    def chain(tile_ref, scales, row, start, stop):
        @pl.loop(start, stop)
        def _(t):
            before = tbl_s[row, BLOCK + t]
            slots[t] = slots[before] + scales[0, t] * tile_ref[t].astype(F32)

    def place(target, row, sources):
        @pl.loop(0, sources // 2)
        def _(s2):
            for b in range(4):
                for s in range(2):
                    final = tbl_s[row, b * sources + s2 * 2 + s]
                    target[s2, b * BLOCK : (b + 1) * BLOCK, s * BLOCK : (s + 1) * BLOCK] = slots[final].astype(BF)

    for device in column + [partner]:
        send(rq, reqs.at[z * 2 + c], qsem.at[z * 2 + c], device)
    for device in across:
        send(rq, reqs.at[8 + c], qsem.at[8 + c], device)
    for py in (yp, ym, y2):
        send(rq, xreqs.at[y], qsem.at[10 + y], dev(x, py, z, c))
    send(rq, xreqs.at[4], qsem.at[14], dev(xnb, y, z, c))
    xa_first(0, init, 0)
    xa_first(0, init, 1)
    zb_first(0, init)
    reqs[z * 2 + c] = rq[...]
    xreqs[y] = rq[...]

    keys[...] = jnp.full((8, 256), -1, I32)
    live = count_ref[0, 0]
    at = lax.broadcasted_iota(I32, (1, TILES), 1)
    keys[0:1, 0:TILES] = jnp.where(at < live, dst_ref[...] * SOURCES + src_ref[...], -1)
    chain_tables(keys, tbl, 2, TILES, 0)
    keys[0:1, 0:256] = jnp.full((1, 256), -1, I32)
    keys[0:1, 0:XTILES] = xdst_ref[...] * XSOURCES + xsrc_ref[...]
    chain_tables(keys, tbl, 1, TILES, 1)
    copy_tbl = pltpu.make_async_copy(tbl, tbl_s, lsem.at[5])
    copy_tbl.start()
    slots[TILES] = jnp.zeros((BLOCK, BLOCK), F32)

    for pz in (zp, zm, z2):
        for pc in range(2):
            arrived(reqs.at[pz * 2 + pc], qsem.at[pz * 2 + pc])
    arrived(reqs.at[z * 2 + 1 - c], qsem.at[z * 2 + 1 - c])
    for pc in range(2):
        arrived(reqs.at[8 + pc], qsem.at[8 + pc])
    copy_req = pltpu.make_async_copy(reqs, reqs_s, lsem.at[6])
    copy_req.start()
    copy_req.wait()

    def begin(e, table):
        za_first(e, OWN, table)
        xb_first(e, 0, table)

    begin(0, init)
    xa_forward(0, 0)
    xa_forward(0, 1)
    zb_forward(0)
    za_rest(0, OWN, init)
    for py in (yp, ym, y2):
        arrived(xreqs.at[py], qsem.at[10 + py])
    arrived(xreqs.at[4], qsem.at[14])
    copy_xreq = pltpu.make_async_copy(xreqs, xreqs_s, lsem.at[7])
    copy_xreq.start()
    copy_tbl.wait()
    loads["tiles0"].wait()
    xb_forward(0, 0)
    zb_done(0)
    xb_first(0, 1)
    xb_first(0, 2)
    chain(tiles, scale_ref, 0, 0, 48)
    xa_done(0)
    za_first(0, ANT, anta[0])
    za_forward(0, OWN)
    za_rest(0, ANT, anta[0])
    chain(tiles, scale_ref, 0, 48, 96)
    zb_far_done(0)
    xb_first(0, 3)
    xb_forward(0, 1)
    xb_forward(0, 2)
    loads["tiles1"].wait()
    chain(tiles, scale_ref, 0, 96, 144)
    xb_forward(0, 3)
    chain(tiles, scale_ref, 0, 144, 192)
    load("xtiles", xtiles_hbm, tiles.at[pl.ds(0, XTILES)], 8)
    za_forward(0, ANT)
    place(adj, 0, SOURCES)
    dot_own(init)
    for key in (3, 0, 1, 2):
        dot_a(0, OWN, key)
    for r in range(4):
        dot_b(0, OWN, r)
        dot_b(0, ANT, r)
    copy_xreq.wait()
    loads["held"].wait()
    loads["weights"].wait()
    for key in (3, 0, 1, 2):
        dot_a(0, ANT, key)
    drain()
    layer(1, held, hbuf.at[0], lambda half: xa_first(1, hbuf.at[0], half))

    h1 = hbuf.at[0]
    zb_first(1, h1)
    begin(1, h1)
    dot_own(h1)
    xa_forward(1, 0)
    xa_forward(1, 1)
    zb_forward(1)
    za_rest(1, OWN, h1)
    xb_forward(1, 0)
    dot_a(1, OWN, 3)
    dot_b(1, OWN, 0)
    zb_done(1)
    xb_first(1, 1)
    xb_first(1, 2)
    xa_done(1)
    za_first(1, ANT, anta[1])
    za_forward(1, OWN)
    za_rest(1, ANT, anta[1])
    dot_b(1, OWN, 1)
    dot_b(1, OWN, 2)
    zb_far_done(1)
    xb_first(1, 3)
    xb_forward(1, 1)
    xb_forward(1, 2)
    dot_b(1, ANT, 0)
    dot_b(1, OWN, 3)
    dot_a(1, OWN, 0)
    dot_a(1, OWN, 1)
    xb_forward(1, 3)
    dot_a(1, OWN, 2)
    dot_a(1, ANT, 3)
    za_forward(1, ANT)
    loads["xtiles"].wait()
    chain(tiles, xscale_ref, 1, 0, XTILES)
    place(xadj, 1, XSOURCES)
    for r in range(1, 4):
        dot_b(1, ANT, r)
    for key in (0, 1, 2):
        dot_a(1, ANT, key)
    drain()

    h2 = hbuf.at[1]

    def na_first(half):
        a = cols_a[2]
        if half == 0:
            send(h2.at[0, :, a], xfo, os.at[0], dev(xot, y, z, c))
            order = (1,)
        else:
            order = (2, 3, 0)
        for k in order:
            send(h2.at[k, :, a], nba.at[k], ns.at[k], dev(xnb, y, z, c))

    def na_forward(k):
        arrived(nba.at[k], ns.at[k])
        send(nba.at[k], anta[2].at[k], asa.at[2, k], dev(xot, y, z, c))

    def no_forward():
        arrived(xfo, os.at[0])
        send(xfo, anta[2].at[0], asa.at[2, 0], dev(xnb, y, z, c))

    def na_done():
        arrived(nba.at[0], ns.at[0])

    def ya_gather(ty, table, g, py, k):
        want = xreqs_s[py, 1 + k, group(y, ty)]
        gxa[ty, g] = table[want, :, cols_a[2]]

    def ya_first(ty, table):
        ya_gather(ty, table, 0, y2, 0)
        send(gxa.at[ty, 0], yfa.at[0, ty], yss.at[0, ty], dev(x, yp, z, c))
        ya_gather(ty, table, 1, y2, 1)
        send(gxa.at[ty, 1], yfa.at[1, ty], yss.at[1, ty], dev(x, ym, z, c))

    def ya_rest(ty, table):
        mine = cra.at[pair(group(y, ty))]
        for i, py in enumerate((yp, ym)):
            ya_gather(ty, table, 2 + 2 * i, py, 0)
            ya_gather(ty, table, 3 + 2 * i, py, 1)
            send(gxa.at[ty, pair(1 + i)], mine, csa.at[i, ty], dev(x, py, z, c))
        for k in range(2):
            want = xreqs_s[y, 1 + k, group(y, ty)]
            cra[group(y, ty) * 2 + k] = table[want, :, cols_a[2]]

    def ya_forward(ty):
        arrived(yfa.at[0, ty], yss.at[0, ty])
        send(yfa.at[0, ty], cra.at[group(ym, ty) * 2], csa.at[2, ty], dev(x, yp, z, c))
        arrived(yfa.at[1, ty], yss.at[1, ty])
        send(yfa.at[1, ty], cra.at[group(yp, ty) * 2 + 1], csa.at[3, ty], dev(x, ym, z, c))

    ysems = {(i, j): yags.at[i, j] for i in range(3) for j in range(2)}
    yring = (yagm, yagp, yagz, ysems, dev(x, yp, z, c), dev(x, ym, z, c))

    def yb_first(r):
        table = (h2, yagm, yagp, yagz)[r]
        g = group(rel_y[r], OWN)
        for k in range(2):
            for row, keep in ((4, False), (y, True)):
                want = xreqs_s[row, 1 + k, g]
                value = table[want, :, cols_b[2]] if r == 0 else table[want]
                if keep:
                    crb[g * 2 + k] = value
                else:
                    gxb[2 * r + k] = value
        send(gxb.at[pl.ds(2 * r, 2)], crb.at[pair(g)], csb.at[r], dev(xnb, y, z, c))

    def cross_a(ty, key, first=False):
        py = (ym, yp, y2, y)[key]
        g = group(py, ty)
        if key < 2:
            arrived(cra.at[pair(g)], csa.at[key, ty])
        if key == 2:
            arrived(cra.at[g * 2], csa.at[2, ty])
            arrived(cra.at[g * 2 + 1], csa.at[3, ty])
        dot_into(xacc, xadj.at[g], cra.at[pair(g)], 0, CA[2], first)

    def cross_b(ty, r, first=False):
        g = group(rel_y[r], ty)
        if ty == ANT:
            arrived(crb.at[pair(g)], csb.at[r])
        dot_into(xacc, xadj.at[g], crb.at[pair(g)], CA[2], CB[2], first)

    layer(2, held, h2, na_first)
    zb_first(2, h2)
    ring_first(h2, cols_b[2], yagm, yagp, ysems, dev(x, yp, z, c), dev(x, ym, z, c))
    za_first(2, OWN, h2)
    ya_first(OWN, h2)
    xb_first(2, 0, h2)
    zb_forward(2)
    ring_forward(*yring)
    za_rest(2, OWN, h2)
    ya_rest(OWN, h2)
    na_forward(1)
    no_forward()
    zb_done(2)
    xb_first(2, 1)
    xb_first(2, 2)
    yb_first(0)
    na_forward(2)
    ring_done(yagm, yagp, ysems)
    yb_first(1)
    yb_first(2)
    dot_own(h2)
    na_forward(3)
    za_forward(2, OWN)
    ya_forward(OWN)
    zb_far_done(2)
    xb_first(2, 3)
    ring_far_done(yagz, ysems)
    yb_first(3)
    na_done()
    ya_first(ANT, nba)
    ya_rest(ANT, nba)
    xb_forward(2, 0)
    cross_a(OWN, 3, first=True)
    cross_a(ANT, 3)
    cross_b(OWN, 0, first=True)
    xb_forward(2, 1)
    xb_forward(2, 2)
    xa_done(2)
    za_first(2, ANT, anta[2])
    za_rest(2, ANT, anta[2])
    xb_forward(2, 3)
    for key in (3, 0, 1):
        dot_a(2, OWN, key)
    cross_a(OWN, 0)
    cross_a(OWN, 1)
    ya_forward(ANT)
    za_forward(2, ANT)
    for r in range(1, 4):
        cross_b(OWN, r)
    dot_a(2, OWN, 2)
    cross_a(OWN, 2)
    for r in range(4):
        dot_b(2, OWN, r)
    dot_a(2, ANT, 3)
    for r in range(4):
        dot_b(2, ANT, r)
        cross_b(ANT, r)
    cross_a(ANT, 0)
    cross_a(ANT, 1)
    dot_a(2, ANT, 0)
    dot_a(2, ANT, 1)
    cross_a(ANT, 2)
    ref_ref[...] = xacc[...].astype(BF)
    dot_a(2, ANT, 2)
    layer(3, ref_ref, out_ref, blocks=False)
    drain()


def finish(a, b, to_a, to_b, held_a, held_b, sem):
    ins = [pltpu.make_async_copy(a, held_a, sem.at[0]), pltpu.make_async_copy(b, held_b, sem.at[1])]
    outs = [pltpu.make_async_copy(held_a, to_a, sem.at[2]), pltpu.make_async_copy(held_b, to_b, sem.at[3])]
    for copy in ins:
        copy.start()
    for copy, out in zip(ins, outs):
        copy.wait()
        out.start()
    for out in outs:
        out.wait()


def per_device(
    initial,
    held_cross,
    weights,
    need_rows,
    tiles,
    tile_scale,
    tile_src,
    tile_dst,
    tile_count,
    cross_need,
    cross_tiles,
    cross_scale,
    cross_src,
    cross_dst,
):
    hbm = pl.BlockSpec(memory_space=pl.ANY)
    vmem = pl.BlockSpec(memory_space=pltpu.VMEM)
    smem = pl.BlockSpec(memory_space=pltpu.SMEM)
    dma = pltpu.SemaphoreType.DMA
    table = jax.ShapeDtypeStruct((ROWS, D), BF)
    out = pl.pallas_call(
        kernel,
        out_shape=(table, table),
        in_specs=[hbm, hbm, hbm, vmem, hbm, smem, vmem, vmem, smem, vmem, hbm, smem, vmem, vmem],
        out_specs=(vmem, vmem),
        scratch_shapes=[
            pltpu.VMEM((4, BLOCK, D), BF),
            pltpu.VMEM((ROWS, D), BF),
            pltpu.VMEM((3, D, D), BF),
            pltpu.VMEM((TILES, BLOCK, BLOCK), BF),
            pltpu.VMEM((TILES + 1, BLOCK, BLOCK), F32),
            pltpu.VMEM((SOURCES // 2, ROWS, 2 * BLOCK), BF),
            pltpu.VMEM((XSOURCES // 2, ROWS, 2 * BLOCK), BF),
            pltpu.VMEM((ROWS, D), F32),
            pltpu.VMEM((ROWS, D), F32),
            pltpu.VMEM((ROWS, D), BF),
            pltpu.VMEM((2, 4, BLOCK, D), BF),
            pltpu.VMEM((16, BLOCK, CA[0]), BF),
            pltpu.VMEM((16, BLOCK, CA[1]), BF),
            pltpu.VMEM((16, BLOCK, CA[2]), BF),
            pltpu.VMEM((16, BLOCK, CB[0]), BF),
            pltpu.VMEM((16, BLOCK, CB[1]), BF),
            pltpu.VMEM((16, BLOCK, CB[2]), BF),
            pltpu.VMEM((4, BLOCK, CA[0]), BF),
            pltpu.VMEM((4, BLOCK, CA[1]), BF),
            pltpu.VMEM((4, BLOCK, CA[2]), BF),
            pltpu.VMEM((2, 2, 2, BLOCK, CA[0]), BF),
            pltpu.VMEM((2, 2, BLOCK, CA[0]), BF),
            pltpu.VMEM((2, 2, BLOCK, CA[1]), BF),
            pltpu.VMEM((2, 2, BLOCK, CA[2]), BF),
            pltpu.VMEM((4, BLOCK, CB[0]), BF),
            pltpu.VMEM((4, BLOCK, CB[1]), BF),
            pltpu.VMEM((4, BLOCK, CB[2]), BF),
            pltpu.VMEM((4, BLOCK, CB[0]), BF),
            pltpu.VMEM((4, BLOCK, CB[1]), BF),
            pltpu.VMEM((4, BLOCK, CB[2]), BF),
            pltpu.VMEM((4, BLOCK, CB[0]), BF),
            pltpu.VMEM((4, BLOCK, CB[1]), BF),
            pltpu.VMEM((4, BLOCK, CB[2]), BF),
            pltpu.VMEM((2, 4, BLOCK, CB[0]), BF),
            pltpu.VMEM((2, 4, BLOCK, CB[1]), BF),
            pltpu.VMEM((2, 4, BLOCK, CB[2]), BF),
            pltpu.VMEM((4, BLOCK, CA[2]), BF),
            pltpu.VMEM((BLOCK, CA[2]), BF),
            pltpu.VMEM((2, 7, BLOCK, CA[0]), BF),
            pltpu.VMEM((2, 7, BLOCK, CA[2]), BF),
            pltpu.VMEM((12, BLOCK, CB[0]), BF),
            pltpu.VMEM((12, BLOCK, CB[2]), BF),
            pltpu.VMEM((16, BLOCK, CA[2]), BF),
            pltpu.VMEM((16, BLOCK, CB[2]), BF),
            pltpu.VMEM((2, 2, BLOCK, CA[2]), BF),
            pltpu.VMEM((2, 6, BLOCK, CA[2]), BF),
            pltpu.VMEM((4, BLOCK, CB[2]), BF),
            pltpu.VMEM((4, BLOCK, CB[2]), BF),
            pltpu.VMEM((4, BLOCK, CB[2]), BF),
            pltpu.VMEM((8, BLOCK, CB[2]), BF),
            pltpu.VMEM((4, BLOCK), I32),
            pltpu.VMEM((10, 4, BLOCK), I32),
            pltpu.VMEM((5, 4, BLOCK), I32),
            pltpu.SMEM((10, 4, BLOCK), I32),
            pltpu.SMEM((5, 4, BLOCK), I32),
            pltpu.VMEM((8, 2 * BLOCK), I32),
            pltpu.VMEM((8, 3 * BLOCK), I32),
            pltpu.SMEM((8, 3 * BLOCK), I32),
            dma((9,)),
            dma((96,)),
            dma((15,)),
            dma((2, 2, 2)),
            dma((3, 4)),
            dma((3, 2, 2)),
            dma((3, 4, 2, 2)),
            dma((3, 3, 2)),
            dma((3, 2, 4)),
            dma((3, 4, 2)),
            dma((3, 4)),
            dma((4,)),
            dma((1,)),
            dma((2, 2)),
            dma((4, 2)),
            dma((3, 2)),
            dma((4,)),
        ],
        compiler_params=pltpu.CompilerParams(
            collective_id=0, has_side_effects=True, vmem_limit_bytes=67043328
        ),
    )(
        initial.reshape(4, BLOCK, D),
        held_cross,
        weights,
        need_rows.reshape(1, 16),
        tiles[0, 0],
        tile_scale[0],
        tile_src[0],
        tile_dst[0],
        tile_count,
        cross_need[0, 0].T,
        cross_tiles[0, 0],
        cross_scale[0],
        cross_src[0],
        cross_dst[0],
    )
    return pl.pallas_call(
        finish,
        out_shape=(table, table),
        in_specs=[hbm, hbm],
        out_specs=(hbm, hbm),
        scratch_shapes=[pltpu.VMEM((ROWS, D), BF)] * 2 + [dma((4,))],
    )(*out)


def solution(mesh):
    in_specs = (
        P(("comm", "dom"), None),
        P(("comm", "dom"), None),
        P(),
        P("comm", "dom", None, None),
        P("comm", "dom", None, None, None),
        P("comm", "dom", None),
        P("comm", "dom", None),
        P("comm", "dom", None),
        P("comm", "dom"),
        P("comm", "dom", None, None),
        P("comm", "dom", None, None, None),
        P("comm", "dom", None),
        P("comm", "dom", None),
        P("comm", "dom", None),
    )
    out_specs = (P(("comm", "dom"), None), P(("comm", "dom"), None))
    return jax.shard_map(
        per_device, mesh=mesh, in_specs=in_specs, out_specs=out_specs, check_vma=False
    )
```

```python
import functools
import math

import jax
import jax.numpy as jnp
from jax import lax
from jax.experimental import pallas as pl
from jax.experimental.pallas import tpu as pltpu
from jax.sharding import PartitionSpec as P

BLOCK = 128
D = 512
ROWS = 512
TILES = 192
XTILES = 64
SOURCES = 20
XSOURCES = 16
ALPHA = 0.1
LAMBDA = 0.5
MESH = pl.DeviceIdType.MESH
BF = jnp.bfloat16
F32 = jnp.float32
I32 = jnp.int32
OWN, ANT = 0, 1
CA = (256, 256, 384)
CB = tuple(D - n for n in CA)


def pair(i):
    return pl.ds(i * 2, 2)


def chain_tables(key_ref, tbl_ref, halves, none, row):
    iota0 = lax.broadcasted_iota(I32, (BLOCK, BLOCK), 0)
    iota1 = lax.broadcasted_iota(I32, (BLOCK, BLOCK), 1)
    last = jnp.full((1, BLOCK), -1, I32)
    prev = [jnp.full((1, BLOCK), -1, I32) for _ in range(halves)]
    for h in range(halves):
        down = jnp.broadcast_to(key_ref[0:1, h * BLOCK : (h + 1) * BLOCK], (BLOCK, BLOCK)).T
        who = iota0 + h * BLOCK
        hit = jnp.where(down == iota1, who, -1)
        last = jnp.maximum(last, jnp.max(hit, axis=0, keepdims=True))
        for j in range(h, halves):
            across = jnp.broadcast_to(key_ref[0:1, j * BLOCK : (j + 1) * BLOCK], (BLOCK, BLOCK))
            same = jnp.logical_and(down == across, who < iota1 + j * BLOCK)
            prev[j] = jnp.maximum(prev[j], jnp.max(jnp.where(same, who, -1), axis=0, keepdims=True))
    tbl_ref[row : row + 1, 0:BLOCK] = jnp.where(last < 0, none, last)
    for j in range(halves):
        tbl_ref[row : row + 1, (j + 1) * BLOCK : (j + 2) * BLOCK] = jnp.where(prev[j] < 0, none, prev[j])


def kernel(
    init_hbm,
    held_hbm,
    weights_hbm,
    need_ref,
    tiles_hbm,
    scale_ref,
    src_ref,
    dst_ref,
    count_ref,
    xneed_ref,
    xtiles_hbm,
    xscale_ref,
    xsrc_ref,
    xdst_ref,
    out_hbm,
    ref_hbm,
    out_ref,
    ref_ref,
    init,
    held,
    weights,
    tiles,
    slots,
    adj,
    xadj,
    acc,
    xacc,
    rounded,
    hbuf,
    rba0,
    rba1,
    rba2,
    rbb0,
    rbb1,
    rbb2,
    anta0,
    anta1,
    anta2,
    xfa,
    zfa0,
    zfa1,
    zfa2,
    agm0,
    agm1,
    agm2,
    agp0,
    agp1,
    agp2,
    agz0,
    agz1,
    agz2,
    xfb0,
    xfb1,
    xfb2,
    nba,
    xfo,
    gba0,
    gba2,
    gbb0,
    gbb2,
    cra,
    crb,
    yfa,
    gxa,
    yagm,
    yagp,
    yagz,
    gxb,
    rq,
    reqs,
    xreqs,
    reqs_s,
    xreqs_s,
    keys,
    tbl,
    tbl_s,
    lsem,
    ssem,
    qsem,
    xsa,
    asa,
    zsa,
    rsa,
    ags,
    xsb,
    rsb,
    rpb,
    ns,
    os,
    yss,
    csa,
    yags,
    csb,
):
    comm = lax.axis_index("comm")
    dom = lax.axis_index("dom")
    y, xl = comm // 2, comm % 2
    z, xh, c = dom // 4, (dom // 2) % 2, dom % 2
    x = xh * 2 + xl

    def dev(px, py, pz, pc):
        return (py * 2 + px % 2, pz * 4 + (px // 2) * 2 + pc)

    xp, xm, x2 = (x + 1) % 4, (x + 3) % 4, (x + 2) % 4
    xnb = xh * 2 + (1 - xl)
    xot = (x + 3 + 2 * xl) % 4
    zp, zm, z2 = (z + 1) % 4, (z + 3) % 4, (z + 2) % 4
    yp, ym, y2 = (y + 1) % 4, (y + 3) % 4, (y + 2) % 4
    rel_z = (z, zm, zp, z2)
    rel_y = (y, ym, yp, y2)
    anta = (anta0, anta1, anta2)
    agm, agp, agz = (agm0, agm1, agm2), (agp0, agp1, agp2), (agz0, agz1, agz2)
    partner = dev(x, y, z, 1 - c)

    rba, rbb = (rba0, rba1, rba2), (rbb0, rbb1, rbb2)
    zfa, xfb = (zfa0, zfa1, zfa2), (xfb0, xfb1, xfb2)
    gba, gbb = (gba0, gba0, gba2), (gbb0, gbb0, gbb2)
    cols_a = tuple(pl.ds(0, n) for n in CA)
    cols_b = tuple(pl.ds(n, D - n) for n in CA)

    loads = {}

    def load(name, src, dst, i):
        loads[name] = pltpu.make_async_copy(src, dst, lsem.at[i])
        loads[name].start()

    load("init", init_hbm, init, 0)
    load("tiles0", tiles_hbm.at[pl.ds(0, 96)], tiles.at[pl.ds(0, 96)], 1)
    load("tiles1", tiles_hbm.at[pl.ds(96, 96)], tiles.at[pl.ds(96, 96)], 2)
    load("held", held_hbm, held, 3)
    load("weights", weights_hbm, weights, 4)

    barrier = pltpu.get_barrier_semaphore()
    column = [dev(x, y, pz, pc) for pz in (zp, zm, z2) for pc in range(2)]
    across = [dev(x2, y, z, pc) for pc in range(2)]
    peers = [dev(xp, y, z, 0), dev(xp, y, z, 1), dev(xm, y, z, 0), dev(xm, y, z, 1), partner] + column + across
    peers += [dev(x, py, z, c) for py in (yp, ym, y2)]
    for peer in peers:
        pl.semaphore_signal(barrier, inc=1, device_id=peer, device_id_type=MESH)
    rq[0:1, 0:16] = need_ref[...]
    rq[1:3, 0:8] = xneed_ref[...]

    keys[...] = jnp.full((8, 256), -1, I32)
    live = count_ref[0, 0]
    at = lax.broadcasted_iota(I32, (1, TILES), 1)
    keys[0:1, 0:TILES] = jnp.where(at < live, dst_ref[...] * SOURCES + src_ref[...], -1)
    chain_tables(keys, tbl, 2, TILES, 0)
    keys[0:1, 0:256] = jnp.full((1, 256), -1, I32)
    keys[0:1, 0:XTILES] = xdst_ref[...] * XSOURCES + xsrc_ref[...]
    chain_tables(keys, tbl, 1, TILES, 1)
    copy_tbl = pltpu.make_async_copy(tbl, tbl_s, lsem.at[5])
    copy_tbl.start()
    slots[TILES] = jnp.zeros((BLOCK, BLOCK), F32)

    loads["init"].wait()
    pl.semaphore_wait(barrier, len(peers))

    sent = []
    used = iter(range(240))

    def send(src, dst, sem, device):
        copy = pltpu.make_async_remote_copy(
            src_ref=src,
            dst_ref=dst,
            send_sem=ssem.at[next(used)],
            recv_sem=sem,
            device_id=device,
            device_id_type=MESH,
        )
        copy.start()
        sent.append(copy)

    def arrived(dst, sem):
        pltpu.make_async_remote_copy(
            src_ref=dst,
            dst_ref=dst,
            send_sem=ssem.at[0],
            recv_sem=sem,
            device_id=partner,
            device_id_type=MESH,
        ).wait_recv()

    def drain(copies):
        for copy in copies:
            copy.wait_send()

    def part(pz, ty, pc):
        return pz * 4 + (xh if ty == OWN else 1 - xh) * 2 + pc

    def group(py, ty):
        return py * 2 + (xl if ty == OWN else 1 - xl)


    def xa_first(e, table, half):
        device = dev(xp, y, z, c) if half == 0 else dev(xm, y, z, c)
        for k in range(2):
            send(table.at[2 * half + k, :, cols_a[e]], xfa.at[e, half, k], xsa.at[e, half, k], device)

    def xa_forward(e, k):
        for half in range(2):
            arrived(xfa.at[e, half, k], xsa.at[e, half, k])
            device = dev(xp, y, z, c) if half == 0 else dev(xm, y, z, c)
            send(xfa.at[e, half, k], anta[e].at[2 * half + k], asa.at[e, 2 * half + k], device)

    def xa_done(e):
        for k in range(4):
            arrived(anta[e].at[k], asa.at[e, k])

    def za_gather(e, ty, table, g, pz, pc, p):
        want = reqs_s[pz * 2 + pc, 0, p]
        gba[e][ty, g] = table[want, :, cols_a[e]]
        return gba[e].at[ty, g]

    def za_first(e, ty, table):
        p = part(z, ty, c)
        send(za_gather(e, ty, table, 0, z2, 0, p), zfa[e].at[0, ty], zsa.at[e, 0, ty], dev(x, y, zp, c))
        send(za_gather(e, ty, table, 1, z2, 1, p), zfa[e].at[1, ty], zsa.at[e, 1, ty], dev(x, y, zm, c))

    def za_rest(e, ty, table):
        p = part(z, ty, c)
        mine = rba[e].at[p]
        send(za_gather(e, ty, table, 2, zp, 0, p), mine, rsa.at[e, 0, ty, c], dev(x, y, zp, 0))
        send(za_gather(e, ty, table, 3, zm, 0, p), mine, rsa.at[e, 1, ty, c], dev(x, y, zm, 0))
        send(za_gather(e, ty, table, 4, zp, 1, p), mine, rsa.at[e, 0, ty, c], dev(x, y, zp, 1))
        send(za_gather(e, ty, table, 5, zm, 1, p), mine, rsa.at[e, 1, ty, c], dev(x, y, zm, 1))
        send(za_gather(e, ty, table, 6, z, 1 - c, p), mine, rsa.at[e, 3, ty, 0], partner)
        want = reqs_s[z * 2 + c, 0, p]
        rba[e][p] = table[want, :, cols_a[e]]

    def za_forward(e, ty):
        arrived(zfa[e].at[0, ty], zsa.at[e, 0, ty])
        send(zfa[e].at[0, ty], rba[e].at[part(zm, ty, c)], rsa.at[e, 2, ty, c], dev(x, y, zp, 0))
        arrived(zfa[e].at[1, ty], zsa.at[e, 1, ty])
        send(zfa[e].at[1, ty], rba[e].at[part(zp, ty, c)], rsa.at[e, 2, ty, c], dev(x, y, zm, 1))


    def ring_first(table, b, fromm, fromp, sems, up, down):
        low, high = pl.ds(0, 2), pl.ds(2, 2)
        send(table.at[low, :, b], fromm.at[low], sems[0, 0], up)
        send(table.at[high, :, b], fromp.at[high], sems[1, 0], down)
        send(table.at[high, :, b], fromm.at[high], sems[0, 1], up)
        send(table.at[low, :, b], fromp.at[low], sems[1, 1], down)

    def ring_forward(fromm, fromp, far, sems, up, down):
        low, high = pl.ds(0, 2), pl.ds(2, 2)
        arrived(fromm.at[low], sems[0, 0])
        send(fromm.at[low], far.at[low], sems[2, 0], up)
        arrived(fromp.at[high], sems[1, 0])
        send(fromp.at[high], far.at[high], sems[2, 1], down)

    def ring_done(fromm, fromp, sems):
        arrived(fromm.at[pl.ds(2, 2)], sems[0, 1])
        arrived(fromp.at[pl.ds(0, 2)], sems[1, 1])

    def ring_far_done(far, sems):
        arrived(far.at[pl.ds(0, 2)], sems[2, 0])
        arrived(far.at[pl.ds(2, 2)], sems[2, 1])

    def zring(e):
        sems = {(i, j): ags.at[e, i, j] for i in range(3) for j in range(2)}
        return agm[e], agp[e], agz[e], sems, dev(x, y, zp, c), dev(x, y, zm, c)

    def zb_first(e, table):
        m, p, _, sems, up, down = zring(e)
        ring_first(table, cols_b[e], m, p, sems, up, down)

    def zb_forward(e):
        ring_forward(*zring(e))

    def zb_done(e):
        m, p, _, sems, _, _ = zring(e)
        ring_done(m, p, sems)

    def zb_far_done(e):
        _, _, far, sems, _, _ = zring(e)
        ring_far_done(far, sems)

    def xb_first(e, r, own=None):
        table = (own, agm[e], agp[e], agz[e])[r]
        p = part(rel_z[r], OWN, c)

        def wanted(row):
            want = reqs_s[row, 0, p]
            return table[want, :, cols_b[e]] if r == 0 else table[want]

        gbb[e][3 * r] = wanted(8)
        send(gbb[e].at[3 * r], xfb[e].at[0, r], xsb.at[e, 0, r], dev(xp, y, z, c))
        gbb[e][3 * r + 1] = wanted(9)
        send(gbb[e].at[3 * r + 1], xfb[e].at[1, r], xsb.at[e, 1, r], dev(xm, y, z, c))
        gbb[e][3 * r + 2] = wanted(z * 2 + 1 - c)
        send(gbb[e].at[3 * r + 2], rbb[e].at[p], rpb.at[e, r], partner)
        rbb[e][p] = wanted(z * 2 + c)

    def xb_forward(e, r):
        arrived(xfb[e].at[0, r], xsb.at[e, 0, r])
        send(xfb[e].at[0, r], rbb[e].at[rel_z[r] * 4 + (xm // 2) * 2 + c], rsb.at[e, r, c], dev(xp, y, z, 0))
        arrived(xfb[e].at[1, r], xsb.at[e, 1, r])
        send(xfb[e].at[1, r], rbb[e].at[rel_z[r] * 4 + (xp // 2) * 2 + c], rsb.at[e, r, c], dev(xm, y, z, 1))


    def dot_into(total, lhs, rhs, start, width, first=False):
        for n in range(0, width, 256):
            w = min(256, width - n)
            cols = pl.ds(start + n, w)
            value = jnp.dot(lhs[...], rhs[:, :, n : n + w].reshape(256, w), preferred_element_type=F32)
            if first:
                total[:, cols] = value
            else:
                total[:, cols] += value

    def dot_own(table):
        dot_into(acc, adj.at[0], table.at[pl.ds(0, 2)], 0, D, first=True)
        dot_into(acc, adj.at[1], table.at[pl.ds(2, 2)], 0, D)

    def dot_a(e, ty, key):
        pz = (zm, zp, z2, z)[key]
        if key == 3:
            arrived(rba[e].at[part(z, ty, 1 - c)], rsa.at[e, 3, ty, 0])
        else:
            for pc in range(2):
                arrived(rba[e].at[part(pz, ty, pc)], rsa.at[e, key, ty, pc])
        j = pz * 2 + (xh if ty == OWN else 1 - xh)
        dot_into(acc, adj.at[2 + j], rba[e].at[pair(j)], 0, CA[e])

    def dot_b(e, ty, r):
        if ty == OWN:
            arrived(rbb[e].at[part(rel_z[r], OWN, 1 - c)], rpb.at[e, r])
        else:
            for pc in range(2):
                arrived(rbb[e].at[part(rel_z[r], ANT, pc)], rsb.at[e, r, pc])
        j = rel_z[r] * 2 + (xh if ty == OWN else 1 - xh)
        dot_into(acc, adj.at[2 + j], rbb[e].at[pair(j)], CA[e], CB[e])

    def layer(level, added, target, after=lambda half: None, blocks=True):
        beta = math.log(LAMBDA / level + 1.0)
        for half in range(2):
            rows = pl.ds(half * 256, 256)
            total = acc[rows, :] + added[rows, :].astype(F32)
            mixed = (1.0 - ALPHA) * total + ALPHA * init[2 * half : 2 * half + 2].reshape(256, D).astype(F32)
            acc[rows, :] = mixed
            rounded[rows, :] = mixed.astype(BF)
            for n in range(2):
                cols = pl.ds(n * 256, 256)
                turned = jnp.dot(rounded[rows, :], weights[level - 1, :, cols], preferred_element_type=F32)
                done = jax.nn.relu((1.0 - beta) * acc[rows, cols] + beta * turned).astype(BF)
                if blocks:
                    target[2 * half : 2 * half + 2, :, cols] = done.reshape(2, BLOCK, 256)
                else:
                    target[rows, cols] = done
            after(half)


    def chain(tile_ref, scales, row, start, stop):
        @pl.loop(start, stop)
        def _(t):
            before = tbl_s[row, BLOCK + t]
            slots[t] = slots[before] + scales[0, t] * tile_ref[t].astype(F32)

    def place(target, row, sources):
        @pl.loop(0, sources // 2)
        def _(s2):
            for b in range(4):
                for s in range(2):
                    final = tbl_s[row, b * sources + s2 * 2 + s]
                    target[s2, b * BLOCK : (b + 1) * BLOCK, s * BLOCK : (s + 1) * BLOCK] = slots[final].astype(BF)

    for device in column + [partner]:
        send(rq, reqs.at[z * 2 + c], qsem.at[z * 2 + c], device)
    for device in across:
        send(rq, reqs.at[8 + c], qsem.at[8 + c], device)
    for py in (yp, ym, y2):
        send(rq, xreqs.at[y], qsem.at[10 + y], dev(x, py, z, c))
    send(rq, xreqs.at[4], qsem.at[14], dev(xnb, y, z, c))
    xa_first(0, init, 0)
    xa_first(0, init, 1)
    zb_first(0, init)
    reqs[z * 2 + c] = rq[...]
    xreqs[y] = rq[...]

    for pz in (zp, zm, z2):
        for pc in range(2):
            arrived(reqs.at[pz * 2 + pc], qsem.at[pz * 2 + pc])
    arrived(reqs.at[z * 2 + 1 - c], qsem.at[z * 2 + 1 - c])
    for pc in range(2):
        arrived(reqs.at[8 + pc], qsem.at[8 + pc])
    copy_req = pltpu.make_async_copy(reqs, reqs_s, lsem.at[6])
    copy_req.start()
    copy_req.wait()

    def begin(e, table):
        za_first(e, OWN, table)
        xb_first(e, 0, table)

    begin(0, init)
    xa_forward(0, 0)
    xa_forward(0, 1)
    zb_forward(0)
    za_rest(0, OWN, init)
    for py in (yp, ym, y2):
        arrived(xreqs.at[py], qsem.at[10 + py])
    arrived(xreqs.at[4], qsem.at[14])
    copy_xreq = pltpu.make_async_copy(xreqs, xreqs_s, lsem.at[7])
    copy_xreq.start()
    copy_tbl.wait()
    loads["tiles0"].wait()
    xb_forward(0, 0)
    zb_done(0)
    xb_first(0, 1)
    xb_first(0, 2)
    chain(tiles, scale_ref, 0, 0, 48)
    xa_done(0)
    za_first(0, ANT, anta[0])
    za_forward(0, OWN)
    za_rest(0, ANT, anta[0])
    chain(tiles, scale_ref, 0, 48, 96)
    zb_far_done(0)
    xb_first(0, 3)
    xb_forward(0, 1)
    xb_forward(0, 2)
    loads["tiles1"].wait()
    chain(tiles, scale_ref, 0, 96, 144)
    xb_forward(0, 3)
    chain(tiles, scale_ref, 0, 144, 192)
    load("xtiles", xtiles_hbm, tiles.at[pl.ds(0, XTILES)], 8)
    za_forward(0, ANT)
    place(adj, 0, SOURCES)
    dot_own(init)
    for key in (3, 0, 1, 2):
        dot_a(0, OWN, key)
    for r in range(4):
        dot_b(0, OWN, r)
        dot_b(0, ANT, r)
    copy_xreq.wait()
    loads["held"].wait()
    loads["weights"].wait()
    for key in (3, 0, 1, 2):
        dot_a(0, ANT, key)
    old = list(sent)
    sent.clear()
    layer(1, held, hbuf.at[0], lambda half: xa_first(1, hbuf.at[0], half))

    h1 = hbuf.at[0]
    zb_first(1, h1)
    drain(old)
    begin(1, h1)
    dot_own(h1)
    xa_forward(1, 0)
    xa_forward(1, 1)
    zb_forward(1)
    za_rest(1, OWN, h1)
    xb_forward(1, 0)
    dot_a(1, OWN, 3)
    dot_b(1, OWN, 0)
    zb_done(1)
    xb_first(1, 1)
    xb_first(1, 2)
    xa_done(1)
    za_first(1, ANT, anta[1])
    za_forward(1, OWN)
    za_rest(1, ANT, anta[1])
    dot_b(1, OWN, 1)
    dot_b(1, OWN, 2)
    zb_far_done(1)
    xb_first(1, 3)
    xb_forward(1, 1)
    xb_forward(1, 2)
    dot_b(1, ANT, 0)
    dot_b(1, OWN, 3)
    dot_a(1, OWN, 0)
    dot_a(1, OWN, 1)
    xb_forward(1, 3)
    dot_a(1, OWN, 2)
    dot_a(1, ANT, 3)
    za_forward(1, ANT)
    loads["xtiles"].wait()
    chain(tiles, xscale_ref, 1, 0, XTILES)
    place(xadj, 1, XSOURCES)
    for r in range(1, 4):
        dot_b(1, ANT, r)
    for key in (0, 1, 2):
        dot_a(1, ANT, key)
    old = list(sent)
    sent.clear()

    h2 = hbuf.at[1]

    def na_first(half):
        a = cols_a[2]
        if half == 0:
            send(h2.at[0, :, a], xfo, os.at[0], dev(xot, y, z, c))
            order = (1,)
        else:
            order = (2, 3, 0)
        for k in order:
            send(h2.at[k, :, a], nba.at[k], ns.at[k], dev(xnb, y, z, c))

    def na_forward(k):
        arrived(nba.at[k], ns.at[k])
        send(nba.at[k], anta[2].at[k], asa.at[2, k], dev(xot, y, z, c))

    def no_forward():
        arrived(xfo, os.at[0])
        send(xfo, anta[2].at[0], asa.at[2, 0], dev(xnb, y, z, c))

    def na_done():
        arrived(nba.at[0], ns.at[0])

    def ya_gather(ty, table, g, py, k):
        want = xreqs_s[py, 1 + k, group(y, ty)]
        gxa[ty, g] = table[want, :, cols_a[2]]

    def ya_first(ty, table):
        ya_gather(ty, table, 0, y2, 0)
        send(gxa.at[ty, 0], yfa.at[0, ty], yss.at[0, ty], dev(x, yp, z, c))
        ya_gather(ty, table, 1, y2, 1)
        send(gxa.at[ty, 1], yfa.at[1, ty], yss.at[1, ty], dev(x, ym, z, c))

    def ya_rest(ty, table):
        mine = cra.at[pair(group(y, ty))]
        for i, py in enumerate((yp, ym)):
            ya_gather(ty, table, 2 + 2 * i, py, 0)
            ya_gather(ty, table, 3 + 2 * i, py, 1)
            send(gxa.at[ty, pair(1 + i)], mine, csa.at[i, ty], dev(x, py, z, c))
        for k in range(2):
            want = xreqs_s[y, 1 + k, group(y, ty)]
            cra[group(y, ty) * 2 + k] = table[want, :, cols_a[2]]

    def ya_forward(ty):
        arrived(yfa.at[0, ty], yss.at[0, ty])
        send(yfa.at[0, ty], cra.at[group(ym, ty) * 2], csa.at[2, ty], dev(x, yp, z, c))
        arrived(yfa.at[1, ty], yss.at[1, ty])
        send(yfa.at[1, ty], cra.at[group(yp, ty) * 2 + 1], csa.at[3, ty], dev(x, ym, z, c))

    ysems = {(i, j): yags.at[i, j] for i in range(3) for j in range(2)}
    yring = (yagm, yagp, yagz, ysems, dev(x, yp, z, c), dev(x, ym, z, c))

    def yb_first(r):
        table = (h2, yagm, yagp, yagz)[r]
        g = group(rel_y[r], OWN)
        for k in range(2):
            for row, keep in ((4, False), (y, True)):
                want = xreqs_s[row, 1 + k, g]
                value = table[want, :, cols_b[2]] if r == 0 else table[want]
                if keep:
                    crb[g * 2 + k] = value
                else:
                    gxb[2 * r + k] = value
        send(gxb.at[pl.ds(2 * r, 2)], crb.at[pair(g)], csb.at[r], dev(xnb, y, z, c))

    def cross_a(ty, key, first=False):
        py = (ym, yp, y2, y)[key]
        g = group(py, ty)
        if key < 2:
            arrived(cra.at[pair(g)], csa.at[key, ty])
        if key == 2:
            arrived(cra.at[g * 2], csa.at[2, ty])
            arrived(cra.at[g * 2 + 1], csa.at[3, ty])
        dot_into(xacc, xadj.at[g], cra.at[pair(g)], 0, CA[2], first)

    def cross_b(ty, r, first=False):
        g = group(rel_y[r], ty)
        if ty == ANT:
            arrived(crb.at[pair(g)], csb.at[r])
        dot_into(xacc, xadj.at[g], crb.at[pair(g)], CA[2], CB[2], first)

    layer(2, held, h2, na_first)
    zb_first(2, h2)
    drain(old)
    ring_first(h2, cols_b[2], yagm, yagp, ysems, dev(x, yp, z, c), dev(x, ym, z, c))
    za_first(2, OWN, h2)
    ya_first(OWN, h2)
    xb_first(2, 0, h2)
    zb_forward(2)
    ring_forward(*yring)
    za_rest(2, OWN, h2)
    ya_rest(OWN, h2)
    na_forward(1)
    no_forward()
    zb_done(2)
    xb_first(2, 1)
    xb_first(2, 2)
    yb_first(0)
    na_forward(2)
    ring_done(yagm, yagp, ysems)
    yb_first(1)
    yb_first(2)
    dot_own(h2)
    na_forward(3)
    za_forward(2, OWN)
    ya_forward(OWN)
    zb_far_done(2)
    xb_first(2, 3)
    ring_far_done(yagz, ysems)
    yb_first(3)
    na_done()
    ya_first(ANT, nba)
    ya_rest(ANT, nba)
    xb_forward(2, 0)
    cross_a(OWN, 3, first=True)
    cross_a(ANT, 3)
    cross_b(OWN, 0, first=True)
    xb_forward(2, 1)
    xb_forward(2, 2)
    xa_done(2)
    za_first(2, ANT, anta[2])
    za_rest(2, ANT, anta[2])
    for key in (3, 0, 1):
        dot_a(2, OWN, key)
    cross_a(OWN, 0)
    cross_a(OWN, 1)
    ya_forward(ANT)
    za_forward(2, ANT)
    xb_forward(2, 3)
    for r in range(1, 4):
        cross_b(OWN, r)
    dot_a(2, OWN, 2)
    cross_a(OWN, 2)
    for r in range(4):
        dot_b(2, OWN, r)
    dot_a(2, ANT, 3)
    for r in range(4):
        dot_b(2, ANT, r)
        cross_b(ANT, r)
    cross_a(ANT, 0)
    cross_a(ANT, 1)
    dot_a(2, ANT, 0)
    dot_a(2, ANT, 1)
    cross_a(ANT, 2)
    ref_ref[...] = xacc[...].astype(BF)
    outs = [pltpu.make_async_copy(ref_ref, ref_hbm, lsem.at[9])]
    outs[0].start()
    dot_a(2, ANT, 2)

    def write(half):
        rows = pl.ds(half * 256, 256)
        outs.append(pltpu.make_async_copy(out_ref.at[rows], out_hbm.at[rows], lsem.at[10 + half]))
        outs[-1].start()

    layer(3, ref_ref, out_ref, write, blocks=False)
    drain(sent)
    for copy in outs:
        copy.wait()


def finish(a, b, to_a, to_b, held_a, held_b, sem):
    ins = [pltpu.make_async_copy(a, held_a, sem.at[0]), pltpu.make_async_copy(b, held_b, sem.at[1])]
    outs = [pltpu.make_async_copy(held_a, to_a, sem.at[2]), pltpu.make_async_copy(held_b, to_b, sem.at[3])]
    for copy in ins:
        copy.start()
    for copy, out in zip(ins, outs):
        copy.wait()
        out.start()
    for out in outs:
        out.wait()


def per_device(
    initial,
    held_cross,
    weights,
    need_rows,
    tiles,
    tile_scale,
    tile_src,
    tile_dst,
    tile_count,
    cross_need,
    cross_tiles,
    cross_scale,
    cross_src,
    cross_dst,
):
    hbm = pl.BlockSpec(memory_space=pl.ANY)
    vmem = pl.BlockSpec(memory_space=pltpu.VMEM)
    smem = pl.BlockSpec(memory_space=pltpu.SMEM)
    dma = pltpu.SemaphoreType.DMA
    table = jax.ShapeDtypeStruct((ROWS, D), BF)
    out = pl.pallas_call(
        kernel,
        out_shape=(table, table),
        in_specs=[hbm, hbm, hbm, vmem, hbm, smem, vmem, vmem, smem, vmem, hbm, smem, vmem, vmem],
        out_specs=(hbm, hbm),
        scratch_shapes=[
            pltpu.VMEM((ROWS, D), BF),
            pltpu.VMEM((ROWS, D), BF),
            pltpu.VMEM((4, BLOCK, D), BF),
            pltpu.VMEM((ROWS, D), BF),
            pltpu.VMEM((3, D, D), BF),
            pltpu.VMEM((TILES, BLOCK, BLOCK), BF),
            pltpu.VMEM((TILES + 1, BLOCK, BLOCK), F32),
            pltpu.VMEM((SOURCES // 2, ROWS, 2 * BLOCK), BF),
            pltpu.VMEM((XSOURCES // 2, ROWS, 2 * BLOCK), BF),
            pltpu.VMEM((ROWS, D), F32),
            pltpu.VMEM((ROWS, D), F32),
            pltpu.VMEM((ROWS, D), BF),
            pltpu.VMEM((2, 4, BLOCK, D), BF),
            pltpu.VMEM((16, BLOCK, CA[0]), BF),
            pltpu.VMEM((16, BLOCK, CA[1]), BF),
            pltpu.VMEM((16, BLOCK, CA[2]), BF),
            pltpu.VMEM((16, BLOCK, CB[0]), BF),
            pltpu.VMEM((16, BLOCK, CB[1]), BF),
            pltpu.VMEM((16, BLOCK, CB[2]), BF),
            pltpu.VMEM((4, BLOCK, CA[0]), BF),
            pltpu.VMEM((4, BLOCK, CA[1]), BF),
            pltpu.VMEM((4, BLOCK, CA[2]), BF),
            pltpu.VMEM((2, 2, 2, BLOCK, CA[0]), BF),
            pltpu.VMEM((2, 2, BLOCK, CA[0]), BF),
            pltpu.VMEM((2, 2, BLOCK, CA[1]), BF),
            pltpu.VMEM((2, 2, BLOCK, CA[2]), BF),
            pltpu.VMEM((4, BLOCK, CB[0]), BF),
            pltpu.VMEM((4, BLOCK, CB[1]), BF),
            pltpu.VMEM((4, BLOCK, CB[2]), BF),
            pltpu.VMEM((4, BLOCK, CB[0]), BF),
            pltpu.VMEM((4, BLOCK, CB[1]), BF),
            pltpu.VMEM((4, BLOCK, CB[2]), BF),
            pltpu.VMEM((4, BLOCK, CB[0]), BF),
            pltpu.VMEM((4, BLOCK, CB[1]), BF),
            pltpu.VMEM((4, BLOCK, CB[2]), BF),
            pltpu.VMEM((2, 4, BLOCK, CB[0]), BF),
            pltpu.VMEM((2, 4, BLOCK, CB[1]), BF),
            pltpu.VMEM((2, 4, BLOCK, CB[2]), BF),
            pltpu.VMEM((4, BLOCK, CA[2]), BF),
            pltpu.VMEM((BLOCK, CA[2]), BF),
            pltpu.VMEM((2, 7, BLOCK, CA[0]), BF),
            pltpu.VMEM((2, 7, BLOCK, CA[2]), BF),
            pltpu.VMEM((12, BLOCK, CB[0]), BF),
            pltpu.VMEM((12, BLOCK, CB[2]), BF),
            pltpu.VMEM((16, BLOCK, CA[2]), BF),
            pltpu.VMEM((16, BLOCK, CB[2]), BF),
            pltpu.VMEM((2, 2, BLOCK, CA[2]), BF),
            pltpu.VMEM((2, 6, BLOCK, CA[2]), BF),
            pltpu.VMEM((4, BLOCK, CB[2]), BF),
            pltpu.VMEM((4, BLOCK, CB[2]), BF),
            pltpu.VMEM((4, BLOCK, CB[2]), BF),
            pltpu.VMEM((8, BLOCK, CB[2]), BF),
            pltpu.VMEM((4, BLOCK), I32),
            pltpu.VMEM((10, 4, BLOCK), I32),
            pltpu.VMEM((5, 4, BLOCK), I32),
            pltpu.SMEM((10, 4, BLOCK), I32),
            pltpu.SMEM((5, 4, BLOCK), I32),
            pltpu.VMEM((8, 2 * BLOCK), I32),
            pltpu.VMEM((8, 3 * BLOCK), I32),
            pltpu.SMEM((8, 3 * BLOCK), I32),
            dma((12,)),
            dma((240,)),
            dma((15,)),
            dma((2, 2, 2)),
            dma((3, 4)),
            dma((3, 2, 2)),
            dma((3, 4, 2, 2)),
            dma((3, 3, 2)),
            dma((3, 2, 4)),
            dma((3, 4, 2)),
            dma((3, 4)),
            dma((4,)),
            dma((1,)),
            dma((2, 2)),
            dma((4, 2)),
            dma((3, 2)),
            dma((4,)),
        ],
        compiler_params=pltpu.CompilerParams(
            collective_id=0, has_side_effects=True, vmem_limit_bytes=67043328
        ),
    )(
        initial.reshape(4, BLOCK, D),
        held_cross,
        weights,
        need_rows.reshape(1, 16),
        tiles[0, 0],
        tile_scale[0],
        tile_src[0],
        tile_dst[0],
        tile_count,
        cross_need[0, 0].T,
        cross_tiles[0, 0],
        cross_scale[0],
        cross_src[0],
        cross_dst[0],
    )
    return pl.pallas_call(
        finish,
        out_shape=(table, table),
        in_specs=[hbm, hbm],
        out_specs=(hbm, hbm),
        scratch_shapes=[pltpu.VMEM((ROWS, D), BF)] * 2 + [dma((4,))],
    )(*out)


def solution(mesh):
    in_specs = (
        P(("comm", "dom"), None),
        P(("comm", "dom"), None),
        P(),
        P("comm", "dom", None, None),
        P("comm", "dom", None, None, None),
        P("comm", "dom", None),
        P("comm", "dom", None),
        P("comm", "dom", None),
        P("comm", "dom"),
        P("comm", "dom", None, None),
        P("comm", "dom", None, None, None),
        P("comm", "dom", None),
        P("comm", "dom", None),
        P("comm", "dom", None),
    )
    out_specs = (P(("comm", "dom"), None), P(("comm", "dom"), None))
    return jax.shard_map(
        per_device, mesh=mesh, in_specs=in_specs, out_specs=out_specs, check_vma=False
    )
```

```python
import functools
import math

import jax
import jax.numpy as jnp
from jax import lax
from jax.experimental import pallas as pl
from jax.experimental.pallas import tpu as pltpu
from jax.sharding import PartitionSpec as P

BLOCK = 128
D = 512
ROWS = 512
TILES = 192
XTILES = 64
SOURCES = 20
XSOURCES = 16
ALPHA = 0.1
LAMBDA = 0.5
MESH = pl.DeviceIdType.MESH
BF = jnp.bfloat16
F32 = jnp.float32
I32 = jnp.int32
OWN, ANT = 0, 1
CA = (256, 256, 384)
CB = tuple(D - n for n in CA)


def pair(i):
    return pl.ds(i * 2, 2)


def chain_tables(key_ref, tbl_ref, halves, none, row):
    iota0 = lax.broadcasted_iota(I32, (BLOCK, BLOCK), 0)
    iota1 = lax.broadcasted_iota(I32, (BLOCK, BLOCK), 1)
    last = jnp.full((1, BLOCK), -1, I32)
    prev = [jnp.full((1, BLOCK), -1, I32) for _ in range(halves)]
    for h in range(halves):
        down = jnp.broadcast_to(key_ref[0:1, h * BLOCK : (h + 1) * BLOCK], (BLOCK, BLOCK)).T
        who = iota0 + h * BLOCK
        hit = jnp.where(down == iota1, who, -1)
        last = jnp.maximum(last, jnp.max(hit, axis=0, keepdims=True))
        for j in range(h, halves):
            across = jnp.broadcast_to(key_ref[0:1, j * BLOCK : (j + 1) * BLOCK], (BLOCK, BLOCK))
            same = jnp.logical_and(down == across, who < iota1 + j * BLOCK)
            prev[j] = jnp.maximum(prev[j], jnp.max(jnp.where(same, who, -1), axis=0, keepdims=True))
    tbl_ref[row : row + 1, 0:BLOCK] = jnp.where(last < 0, none, last)
    for j in range(halves):
        tbl_ref[row : row + 1, (j + 1) * BLOCK : (j + 2) * BLOCK] = jnp.where(prev[j] < 0, none, prev[j])


def kernel(
    init_hbm,
    held_hbm,
    weights_hbm,
    need_ref,
    tiles_hbm,
    scale_ref,
    src_ref,
    dst_ref,
    count_ref,
    xneed_ref,
    xtiles_hbm,
    xscale_ref,
    xsrc_ref,
    xdst_ref,
    out_hbm,
    ref_hbm,
    out_ref,
    ref_ref,
    init,
    held,
    weights,
    tiles,
    slots,
    adj,
    xadj,
    acc,
    xacc,
    rounded,
    hbuf,
    rba0,
    rba1,
    rba2,
    rbb0,
    rbb1,
    rbb2,
    anta0,
    anta1,
    anta2,
    xfa,
    zfa0,
    zfa1,
    zfa2,
    agm0,
    agm1,
    agm2,
    agp0,
    agp1,
    agp2,
    agz0,
    agz1,
    agz2,
    xfb0,
    xfb1,
    xfb2,
    nba,
    xfo,
    gba0,
    gba2,
    gbb0,
    gbb2,
    cra,
    crb,
    yfa,
    gxa,
    yagm,
    yagp,
    yagz,
    gxb,
    rq,
    reqs,
    xreqs,
    reqs_s,
    xreqs_s,
    keys,
    tbl,
    tbl_s,
    lsem,
    ssem,
    qsem,
    xsa,
    asa,
    zsa,
    rsa,
    ags,
    xsb,
    rsb,
    rpb,
    ns,
    os,
    yss,
    csa,
    yags,
    csb,
):
    comm = lax.axis_index("comm")
    dom = lax.axis_index("dom")
    y, xl = comm // 2, comm % 2
    z, xh, c = dom // 4, (dom // 2) % 2, dom % 2
    x = xh * 2 + xl

    def dev(px, py, pz, pc):
        return (py * 2 + px % 2, pz * 4 + (px // 2) * 2 + pc)

    xp, xm, x2 = (x + 1) % 4, (x + 3) % 4, (x + 2) % 4
    xnb = xh * 2 + (1 - xl)
    xot = (x + 3 + 2 * xl) % 4
    zp, zm, z2 = (z + 1) % 4, (z + 3) % 4, (z + 2) % 4
    yp, ym, y2 = (y + 1) % 4, (y + 3) % 4, (y + 2) % 4
    rel_z = (z, zm, zp, z2)
    rel_y = (y, ym, yp, y2)
    anta = (anta0, anta1, anta2)
    agm, agp, agz = (agm0, agm1, agm2), (agp0, agp1, agp2), (agz0, agz1, agz2)
    partner = dev(x, y, z, 1 - c)

    rba, rbb = (rba0, rba1, rba2), (rbb0, rbb1, rbb2)
    zfa, xfb = (zfa0, zfa1, zfa2), (xfb0, xfb1, xfb2)
    gba, gbb = (gba0, gba0, gba2), (gbb0, gbb0, gbb2)
    cols_a = tuple(pl.ds(0, n) for n in CA)
    cols_b = tuple(pl.ds(n, D - n) for n in CA)

    loads = {}

    def load(name, src, dst, i):
        loads[name] = pltpu.make_async_copy(src, dst, lsem.at[i])
        loads[name].start()

    load("init", init_hbm, init, 0)
    load("tiles0", tiles_hbm.at[pl.ds(0, 96)], tiles.at[pl.ds(0, 96)], 1)
    load("tiles1", tiles_hbm.at[pl.ds(96, 96)], tiles.at[pl.ds(96, 96)], 2)
    load("held", held_hbm, held, 3)
    load("weights", weights_hbm, weights, 4)

    barrier = pltpu.get_barrier_semaphore()
    column = [dev(x, y, pz, pc) for pz in (zp, zm, z2) for pc in range(2)]
    across = [dev(x2, y, z, pc) for pc in range(2)]
    peers = [dev(xp, y, z, c), dev(xm, y, z, c), dev((x + 3 - 2 * c) % 4, y, z, 1 - c), partner] + column + across
    peers += [dev(x, py, z, c) for py in (yp, ym, y2)]
    for peer in peers:
        pl.semaphore_signal(barrier, inc=1, device_id=peer, device_id_type=MESH)
    rq[0:1, 0:16] = need_ref[...]
    rq[1:3, 0:8] = xneed_ref[...]

    keys[...] = jnp.full((8, 256), -1, I32)
    live = count_ref[0, 0]
    at = lax.broadcasted_iota(I32, (1, TILES), 1)
    keys[0:1, 0:TILES] = jnp.where(at < live, dst_ref[...] * SOURCES + src_ref[...], -1)
    chain_tables(keys, tbl, 2, TILES, 0)
    keys[0:1, 0:256] = jnp.full((1, 256), -1, I32)
    keys[0:1, 0:XTILES] = xdst_ref[...] * XSOURCES + xsrc_ref[...]
    chain_tables(keys, tbl, 1, TILES, 1)
    copy_tbl = pltpu.make_async_copy(tbl, tbl_s, lsem.at[5])
    copy_tbl.start()
    slots[TILES] = jnp.zeros((BLOCK, BLOCK), F32)

    loads["init"].wait()
    pl.semaphore_wait(barrier, len(peers))

    sent = []
    used = iter(range(240))

    def send(src, dst, sem, device):
        copy = pltpu.make_async_remote_copy(
            src_ref=src,
            dst_ref=dst,
            send_sem=ssem.at[next(used)],
            recv_sem=sem,
            device_id=device,
            device_id_type=MESH,
        )
        copy.start()
        sent.append(copy)

    def arrived(dst, sem):
        pltpu.make_async_remote_copy(
            src_ref=dst,
            dst_ref=dst,
            send_sem=ssem.at[0],
            recv_sem=sem,
            device_id=partner,
            device_id_type=MESH,
        ).wait_recv()

    def drain(copies):
        for copy in copies:
            copy.wait_send()

    def part(pz, ty, pc):
        return pz * 4 + (xh if ty == OWN else 1 - xh) * 2 + pc

    def group(py, ty):
        return py * 2 + (xl if ty == OWN else 1 - xl)


    def xa_first(e, table, half):
        device = dev(xp, y, z, c) if half == 0 else dev(xm, y, z, c)
        for k in range(2):
            send(table.at[2 * half + k, :, cols_a[e]], xfa.at[e, half, k], xsa.at[e, half, k], device)

    def xa_forward(e, k):
        for half in range(2):
            arrived(xfa.at[e, half, k], xsa.at[e, half, k])
            device = dev(xp, y, z, c) if half == 0 else dev(xm, y, z, c)
            send(xfa.at[e, half, k], anta[e].at[2 * half + k], asa.at[e, 2 * half + k], device)

    def xa_done(e):
        for k in range(4):
            arrived(anta[e].at[k], asa.at[e, k])

    def za_gather(e, ty, table, g, pz, pc, p):
        want = reqs_s[pz * 2 + pc, 0, p]
        gba[e][ty, g] = table[want, :, cols_a[e]]
        return gba[e].at[ty, g]

    def za_first(e, ty, table):
        p = part(z, ty, c)
        send(za_gather(e, ty, table, 0, z2, 0, p), zfa[e].at[0, ty], zsa.at[e, 0, ty], dev(x, y, zp, c))
        send(za_gather(e, ty, table, 1, z2, 1, p), zfa[e].at[1, ty], zsa.at[e, 1, ty], dev(x, y, zm, c))

    def za_rest(e, ty, table):
        p = part(z, ty, c)
        mine = rba[e].at[p]
        send(za_gather(e, ty, table, 2, zp, 0, p), mine, rsa.at[e, 0, ty, c], dev(x, y, zp, 0))
        send(za_gather(e, ty, table, 3, zm, 0, p), mine, rsa.at[e, 1, ty, c], dev(x, y, zm, 0))
        send(za_gather(e, ty, table, 4, zp, 1, p), mine, rsa.at[e, 0, ty, c], dev(x, y, zp, 1))
        send(za_gather(e, ty, table, 5, zm, 1, p), mine, rsa.at[e, 1, ty, c], dev(x, y, zm, 1))
        send(za_gather(e, ty, table, 6, z, 1 - c, p), mine, rsa.at[e, 3, ty, 0], partner)
        want = reqs_s[z * 2 + c, 0, p]
        rba[e][p] = table[want, :, cols_a[e]]

    def za_forward(e, ty):
        arrived(zfa[e].at[0, ty], zsa.at[e, 0, ty])
        send(zfa[e].at[0, ty], rba[e].at[part(zm, ty, c)], rsa.at[e, 2, ty, c], dev(x, y, zp, 0))
        arrived(zfa[e].at[1, ty], zsa.at[e, 1, ty])
        send(zfa[e].at[1, ty], rba[e].at[part(zp, ty, c)], rsa.at[e, 2, ty, c], dev(x, y, zm, 1))


    def ring_first(table, b, fromm, fromp, sems, up, down):
        low, high = pl.ds(0, 2), pl.ds(2, 2)
        send(table.at[low, :, b], fromm.at[low], sems[0, 0], up)
        send(table.at[high, :, b], fromp.at[high], sems[1, 0], down)
        send(table.at[high, :, b], fromm.at[high], sems[0, 1], up)
        send(table.at[low, :, b], fromp.at[low], sems[1, 1], down)

    def ring_forward(fromm, fromp, far, sems, up, down):
        low, high = pl.ds(0, 2), pl.ds(2, 2)
        arrived(fromm.at[low], sems[0, 0])
        send(fromm.at[low], far.at[low], sems[2, 0], up)
        arrived(fromp.at[high], sems[1, 0])
        send(fromp.at[high], far.at[high], sems[2, 1], down)

    def ring_done(fromm, fromp, sems):
        arrived(fromm.at[pl.ds(2, 2)], sems[0, 1])
        arrived(fromp.at[pl.ds(0, 2)], sems[1, 1])

    def ring_far_done(far, sems):
        arrived(far.at[pl.ds(0, 2)], sems[2, 0])
        arrived(far.at[pl.ds(2, 2)], sems[2, 1])

    def zring(e):
        sems = {(i, j): ags.at[e, i, j] for i in range(3) for j in range(2)}
        return agm[e], agp[e], agz[e], sems, dev(x, y, zp, c), dev(x, y, zm, c)

    def zb_first(e, table):
        m, p, _, sems, up, down = zring(e)
        ring_first(table, cols_b[e], m, p, sems, up, down)

    def zb_forward(e):
        ring_forward(*zring(e))

    def zb_done(e):
        m, p, _, sems, _, _ = zring(e)
        ring_done(m, p, sems)

    def zb_far_done(e):
        _, _, far, sems, _, _ = zring(e)
        ring_far_done(far, sems)

    def xb_first(e, r, own=None):
        table = (own, agm[e], agp[e], agz[e])[r]
        p = part(rel_z[r], OWN, c)

        def wanted(row):
            want = reqs_s[row, 0, p]
            return table[want, :, cols_b[e]] if r == 0 else table[want]

        gbb[e][3 * r] = wanted(8)
        send(gbb[e].at[3 * r], xfb[e].at[0, r], xsb.at[e, 0, r], dev(xp, y, z, c))
        gbb[e][3 * r + 1] = wanted(9)
        send(gbb[e].at[3 * r + 1], xfb[e].at[1, r], xsb.at[e, 1, r], dev(xm, y, z, c))
        gbb[e][3 * r + 2] = wanted(z * 2 + 1 - c)
        send(gbb[e].at[3 * r + 2], rbb[e].at[p], rpb.at[e, r], partner)
        rbb[e][p] = wanted(z * 2 + c)

    def xb_forward(e, r):
        arrived(xfb[e].at[0, r], xsb.at[e, 0, r])
        send(xfb[e].at[0, r], rbb[e].at[rel_z[r] * 4 + (xm // 2) * 2 + c], rsb.at[e, r, c], dev(xp, y, z, 0))
        arrived(xfb[e].at[1, r], xsb.at[e, 1, r])
        send(xfb[e].at[1, r], rbb[e].at[rel_z[r] * 4 + (xp // 2) * 2 + c], rsb.at[e, r, c], dev(xm, y, z, 1))


    def dot_into(total, lhs, rhs, start, width, first=False):
        for n in range(0, width, 256):
            w = min(256, width - n)
            cols = pl.ds(start + n, w)
            value = jnp.dot(lhs[...], rhs[:, :, n : n + w].reshape(256, w), preferred_element_type=F32)
            if first:
                total[:, cols] = value
            else:
                total[:, cols] += value

    def dot_own(table):
        dot_into(acc, adj.at[0], table.at[pl.ds(0, 2)], 0, D, first=True)
        dot_into(acc, adj.at[1], table.at[pl.ds(2, 2)], 0, D)

    def dot_a(e, ty, key):
        pz = (zm, zp, z2, z)[key]
        if key == 3:
            arrived(rba[e].at[part(z, ty, 1 - c)], rsa.at[e, 3, ty, 0])
        else:
            for pc in range(2):
                arrived(rba[e].at[part(pz, ty, pc)], rsa.at[e, key, ty, pc])
        j = pz * 2 + (xh if ty == OWN else 1 - xh)
        dot_into(acc, adj.at[2 + j], rba[e].at[pair(j)], 0, CA[e])

    def dot_b(e, ty, r):
        if ty == OWN:
            arrived(rbb[e].at[part(rel_z[r], OWN, 1 - c)], rpb.at[e, r])
        else:
            for pc in range(2):
                arrived(rbb[e].at[part(rel_z[r], ANT, pc)], rsb.at[e, r, pc])
        j = rel_z[r] * 2 + (xh if ty == OWN else 1 - xh)
        dot_into(acc, adj.at[2 + j], rbb[e].at[pair(j)], CA[e], CB[e])

    def layer(level, added, target, after=lambda half: None, blocks=True):
        beta = math.log(LAMBDA / level + 1.0)
        for half in range(2):
            rows = pl.ds(half * 256, 256)
            total = acc[rows, :] + added[rows, :].astype(F32)
            mixed = (1.0 - ALPHA) * total + ALPHA * init[2 * half : 2 * half + 2].reshape(256, D).astype(F32)
            acc[rows, :] = mixed
            rounded[rows, :] = mixed.astype(BF)
            for n in range(2):
                cols = pl.ds(n * 256, 256)
                turned = jnp.dot(rounded[rows, :], weights[level - 1, :, cols], preferred_element_type=F32)
                done = jax.nn.relu((1.0 - beta) * acc[rows, cols] + beta * turned).astype(BF)
                if blocks:
                    target[2 * half : 2 * half + 2, :, cols] = done.reshape(2, BLOCK, 256)
                else:
                    target[rows, cols] = done
            after(half)


    def chain(tile_ref, scales, row, start, stop):
        @pl.loop(start, stop)
        def _(t):
            before = tbl_s[row, BLOCK + t]
            slots[t] = slots[before] + scales[0, t] * tile_ref[t].astype(F32)

    def place(target, row, sources):
        @pl.loop(0, sources // 2)
        def _(s2):
            for b in range(4):
                for s in range(2):
                    final = tbl_s[row, b * sources + s2 * 2 + s]
                    target[s2, b * BLOCK : (b + 1) * BLOCK, s * BLOCK : (s + 1) * BLOCK] = slots[final].astype(BF)

    for device in column + [partner]:
        send(rq, reqs.at[z * 2 + c], qsem.at[z * 2 + c], device)
    for device in across:
        send(rq, reqs.at[8 + c], qsem.at[8 + c], device)
    for py in (yp, ym, y2):
        send(rq, xreqs.at[y], qsem.at[10 + y], dev(x, py, z, c))
    send(rq, xreqs.at[4], qsem.at[14], dev(xnb, y, z, c))
    xa_first(0, init, 0)
    xa_first(0, init, 1)
    zb_first(0, init)
    reqs[z * 2 + c] = rq[...]
    xreqs[y] = rq[...]

    for pz in (zp, zm, z2):
        for pc in range(2):
            arrived(reqs.at[pz * 2 + pc], qsem.at[pz * 2 + pc])
    arrived(reqs.at[z * 2 + 1 - c], qsem.at[z * 2 + 1 - c])
    for pc in range(2):
        arrived(reqs.at[8 + pc], qsem.at[8 + pc])
    copy_req = pltpu.make_async_copy(reqs, reqs_s, lsem.at[6])
    copy_req.start()
    copy_req.wait()

    def begin(e, table):
        za_first(e, OWN, table)
        xb_first(e, 0, table)

    begin(0, init)
    xa_forward(0, 0)
    xa_forward(0, 1)
    zb_forward(0)
    za_rest(0, OWN, init)
    for py in (yp, ym, y2):
        arrived(xreqs.at[py], qsem.at[10 + py])
    arrived(xreqs.at[4], qsem.at[14])
    copy_xreq = pltpu.make_async_copy(xreqs, xreqs_s, lsem.at[7])
    copy_xreq.start()
    copy_tbl.wait()
    loads["tiles0"].wait()
    xb_forward(0, 0)
    zb_done(0)
    xb_first(0, 1)
    xb_first(0, 2)
    chain(tiles, scale_ref, 0, 0, 48)
    xa_done(0)
    za_first(0, ANT, anta[0])
    za_forward(0, OWN)
    za_rest(0, ANT, anta[0])
    chain(tiles, scale_ref, 0, 48, 96)
    zb_far_done(0)
    xb_first(0, 3)
    xb_forward(0, 1)
    xb_forward(0, 2)
    loads["tiles1"].wait()
    chain(tiles, scale_ref, 0, 96, 144)
    xb_forward(0, 3)
    chain(tiles, scale_ref, 0, 144, 192)
    load("xtiles", xtiles_hbm, tiles.at[pl.ds(0, XTILES)], 8)
    za_forward(0, ANT)
    place(adj, 0, SOURCES)
    dot_own(init)
    for key in (3, 0, 1, 2):
        dot_a(0, OWN, key)
    for r in range(4):
        dot_b(0, OWN, r)
        dot_b(0, ANT, r)
    copy_xreq.wait()
    loads["held"].wait()
    loads["weights"].wait()
    for key in (3, 0, 1, 2):
        dot_a(0, ANT, key)
    old = list(sent)
    sent.clear()
    layer(1, held, hbuf.at[0], lambda half: xa_first(1, hbuf.at[0], half))

    h1 = hbuf.at[0]
    zb_first(1, h1)
    drain(old)
    begin(1, h1)
    dot_own(h1)
    xa_forward(1, 0)
    xa_forward(1, 1)
    zb_forward(1)
    za_rest(1, OWN, h1)
    xb_forward(1, 0)
    dot_a(1, OWN, 3)
    dot_b(1, OWN, 0)
    zb_done(1)
    xb_first(1, 1)
    xb_first(1, 2)
    xa_done(1)
    za_first(1, ANT, anta[1])
    za_forward(1, OWN)
    za_rest(1, ANT, anta[1])
    dot_b(1, OWN, 1)
    dot_b(1, OWN, 2)
    zb_far_done(1)
    xb_first(1, 3)
    xb_forward(1, 1)
    xb_forward(1, 2)
    dot_b(1, ANT, 0)
    dot_b(1, OWN, 3)
    dot_a(1, OWN, 0)
    dot_a(1, OWN, 1)
    xb_forward(1, 3)
    dot_a(1, OWN, 2)
    dot_a(1, ANT, 3)
    za_forward(1, ANT)
    loads["xtiles"].wait()
    chain(tiles, xscale_ref, 1, 0, XTILES)
    place(xadj, 1, XSOURCES)
    for r in range(1, 4):
        dot_b(1, ANT, r)
    for key in (0, 1, 2):
        dot_a(1, ANT, key)
    old = list(sent)
    sent.clear()

    h2 = hbuf.at[1]

    def na_first(half):
        a = cols_a[2]
        if half == 0:
            send(h2.at[0, :, a], xfo, os.at[0], dev(xot, y, z, c))
            order = (1,)
        else:
            order = (2, 3, 0)
        for k in order:
            send(h2.at[k, :, a], nba.at[k], ns.at[k], dev(xnb, y, z, c))

    def na_forward(k):
        arrived(nba.at[k], ns.at[k])
        send(nba.at[k], anta[2].at[k], asa.at[2, k], dev(xot, y, z, c))

    def no_forward():
        arrived(xfo, os.at[0])
        send(xfo, anta[2].at[0], asa.at[2, 0], dev(xnb, y, z, c))

    def na_done():
        arrived(nba.at[0], ns.at[0])

    def ya_gather(ty, table, g, py, k):
        want = xreqs_s[py, 1 + k, group(y, ty)]
        gxa[ty, g] = table[want, :, cols_a[2]]

    def ya_first(ty, table):
        ya_gather(ty, table, 0, y2, 0)
        send(gxa.at[ty, 0], yfa.at[0, ty], yss.at[0, ty], dev(x, yp, z, c))
        ya_gather(ty, table, 1, y2, 1)
        send(gxa.at[ty, 1], yfa.at[1, ty], yss.at[1, ty], dev(x, ym, z, c))

    def ya_rest(ty, table):
        mine = cra.at[pair(group(y, ty))]
        for i, py in enumerate((yp, ym)):
            ya_gather(ty, table, 2 + 2 * i, py, 0)
            ya_gather(ty, table, 3 + 2 * i, py, 1)
            send(gxa.at[ty, pair(1 + i)], mine, csa.at[i, ty], dev(x, py, z, c))
        for k in range(2):
            want = xreqs_s[y, 1 + k, group(y, ty)]
            cra[group(y, ty) * 2 + k] = table[want, :, cols_a[2]]

    def ya_forward(ty):
        arrived(yfa.at[0, ty], yss.at[0, ty])
        send(yfa.at[0, ty], cra.at[group(ym, ty) * 2], csa.at[2, ty], dev(x, yp, z, c))
        arrived(yfa.at[1, ty], yss.at[1, ty])
        send(yfa.at[1, ty], cra.at[group(yp, ty) * 2 + 1], csa.at[3, ty], dev(x, ym, z, c))

    ysems = {(i, j): yags.at[i, j] for i in range(3) for j in range(2)}
    yring = (yagm, yagp, yagz, ysems, dev(x, yp, z, c), dev(x, ym, z, c))

    def yb_first(r):
        table = (h2, yagm, yagp, yagz)[r]
        g = group(rel_y[r], OWN)
        for k in range(2):
            for row, keep in ((4, False), (y, True)):
                want = xreqs_s[row, 1 + k, g]
                value = table[want, :, cols_b[2]] if r == 0 else table[want]
                if keep:
                    crb[g * 2 + k] = value
                else:
                    gxb[2 * r + k] = value
        send(gxb.at[pl.ds(2 * r, 2)], crb.at[pair(g)], csb.at[r], dev(xnb, y, z, c))

    def cross_a(ty, key, first=False):
        py = (ym, yp, y2, y)[key]
        g = group(py, ty)
        if key < 2:
            arrived(cra.at[pair(g)], csa.at[key, ty])
        if key == 2:
            arrived(cra.at[g * 2], csa.at[2, ty])
            arrived(cra.at[g * 2 + 1], csa.at[3, ty])
        dot_into(xacc, xadj.at[g], cra.at[pair(g)], 0, CA[2], first)

    def cross_b(ty, r, first=False):
        g = group(rel_y[r], ty)
        if ty == ANT:
            arrived(crb.at[pair(g)], csb.at[r])
        dot_into(xacc, xadj.at[g], crb.at[pair(g)], CA[2], CB[2], first)

    layer(2, held, h2, na_first)
    zb_first(2, h2)
    drain(old)
    ring_first(h2, cols_b[2], yagm, yagp, ysems, dev(x, yp, z, c), dev(x, ym, z, c))
    za_first(2, OWN, h2)
    ya_first(OWN, h2)
    xb_first(2, 0, h2)
    zb_forward(2)
    ring_forward(*yring)
    za_rest(2, OWN, h2)
    ya_rest(OWN, h2)
    na_forward(1)
    no_forward()
    zb_done(2)
    xb_first(2, 1)
    xb_first(2, 2)
    yb_first(0)
    na_forward(2)
    ring_done(yagm, yagp, ysems)
    yb_first(1)
    yb_first(2)
    dot_own(h2)
    na_forward(3)
    za_forward(2, OWN)
    ya_forward(OWN)
    zb_far_done(2)
    xb_first(2, 3)
    ring_far_done(yagz, ysems)
    yb_first(3)
    na_done()
    ya_first(ANT, nba)
    ya_rest(ANT, nba)
    xb_forward(2, 0)
    cross_a(OWN, 3, first=True)
    cross_a(ANT, 3)
    cross_b(OWN, 0, first=True)
    xb_forward(2, 1)
    xb_forward(2, 2)
    xa_done(2)
    za_first(2, ANT, anta[2])
    za_rest(2, ANT, anta[2])
    for key in (3, 0, 1):
        dot_a(2, OWN, key)
    cross_a(OWN, 0)
    cross_a(OWN, 1)
    ya_forward(ANT)
    za_forward(2, ANT)
    xb_forward(2, 3)
    for r in range(1, 4):
        cross_b(OWN, r)
    dot_a(2, OWN, 2)
    cross_a(OWN, 2)
    for r in range(4):
        dot_b(2, OWN, r)
    dot_a(2, ANT, 3)
    for r in range(4):
        dot_b(2, ANT, r)
        cross_b(ANT, r)
    cross_a(ANT, 0)
    cross_a(ANT, 1)
    dot_a(2, ANT, 0)
    dot_a(2, ANT, 1)
    cross_a(ANT, 2)
    ref_ref[...] = xacc[...].astype(BF)
    outs = [pltpu.make_async_copy(ref_ref, ref_hbm, lsem.at[9])]
    outs[0].start()
    dot_a(2, ANT, 2)

    def write(half):
        rows = pl.ds(half * 256, 256)
        outs.append(pltpu.make_async_copy(out_ref.at[rows], out_hbm.at[rows], lsem.at[10 + half]))
        outs[-1].start()

    layer(3, ref_ref, out_ref, write, blocks=False)
    drain(sent)
    for copy in outs:
        copy.wait()


def finish(a, b, to_a, to_b, held_a, held_b, sem):
    ins = [pltpu.make_async_copy(a, held_a, sem.at[0]), pltpu.make_async_copy(b, held_b, sem.at[1])]
    outs = [pltpu.make_async_copy(held_a, to_a, sem.at[2]), pltpu.make_async_copy(held_b, to_b, sem.at[3])]
    for copy in ins:
        copy.start()
    for copy, out in zip(ins, outs):
        copy.wait()
        out.start()
    for out in outs:
        out.wait()


def per_device(
    initial,
    held_cross,
    weights,
    need_rows,
    tiles,
    tile_scale,
    tile_src,
    tile_dst,
    tile_count,
    cross_need,
    cross_tiles,
    cross_scale,
    cross_src,
    cross_dst,
):
    hbm = pl.BlockSpec(memory_space=pl.ANY)
    vmem = pl.BlockSpec(memory_space=pltpu.VMEM)
    smem = pl.BlockSpec(memory_space=pltpu.SMEM)
    dma = pltpu.SemaphoreType.DMA
    table = jax.ShapeDtypeStruct((ROWS, D), BF)
    out = pl.pallas_call(
        kernel,
        out_shape=(table, table),
        in_specs=[hbm, hbm, hbm, vmem, hbm, smem, vmem, vmem, smem, vmem, hbm, smem, vmem, vmem],
        out_specs=(hbm, hbm),
        scratch_shapes=[
            pltpu.VMEM((ROWS, D), BF),
            pltpu.VMEM((ROWS, D), BF),
            pltpu.VMEM((4, BLOCK, D), BF),
            pltpu.VMEM((ROWS, D), BF),
            pltpu.VMEM((3, D, D), BF),
            pltpu.VMEM((TILES, BLOCK, BLOCK), BF),
            pltpu.VMEM((TILES + 1, BLOCK, BLOCK), F32),
            pltpu.VMEM((SOURCES // 2, ROWS, 2 * BLOCK), BF),
            pltpu.VMEM((XSOURCES // 2, ROWS, 2 * BLOCK), BF),
            pltpu.VMEM((ROWS, D), F32),
            pltpu.VMEM((ROWS, D), F32),
            pltpu.VMEM((ROWS, D), BF),
            pltpu.VMEM((2, 4, BLOCK, D), BF),
            pltpu.VMEM((16, BLOCK, CA[0]), BF),
            pltpu.VMEM((16, BLOCK, CA[1]), BF),
            pltpu.VMEM((16, BLOCK, CA[2]), BF),
            pltpu.VMEM((16, BLOCK, CB[0]), BF),
            pltpu.VMEM((16, BLOCK, CB[1]), BF),
            pltpu.VMEM((16, BLOCK, CB[2]), BF),
            pltpu.VMEM((4, BLOCK, CA[0]), BF),
            pltpu.VMEM((4, BLOCK, CA[1]), BF),
            pltpu.VMEM((4, BLOCK, CA[2]), BF),
            pltpu.VMEM((2, 2, 2, BLOCK, CA[0]), BF),
            pltpu.VMEM((2, 2, BLOCK, CA[0]), BF),
            pltpu.VMEM((2, 2, BLOCK, CA[1]), BF),
            pltpu.VMEM((2, 2, BLOCK, CA[2]), BF),
            pltpu.VMEM((4, BLOCK, CB[0]), BF),
            pltpu.VMEM((4, BLOCK, CB[1]), BF),
            pltpu.VMEM((4, BLOCK, CB[2]), BF),
            pltpu.VMEM((4, BLOCK, CB[0]), BF),
            pltpu.VMEM((4, BLOCK, CB[1]), BF),
            pltpu.VMEM((4, BLOCK, CB[2]), BF),
            pltpu.VMEM((4, BLOCK, CB[0]), BF),
            pltpu.VMEM((4, BLOCK, CB[1]), BF),
            pltpu.VMEM((4, BLOCK, CB[2]), BF),
            pltpu.VMEM((2, 4, BLOCK, CB[0]), BF),
            pltpu.VMEM((2, 4, BLOCK, CB[1]), BF),
            pltpu.VMEM((2, 4, BLOCK, CB[2]), BF),
            pltpu.VMEM((4, BLOCK, CA[2]), BF),
            pltpu.VMEM((BLOCK, CA[2]), BF),
            pltpu.VMEM((2, 7, BLOCK, CA[0]), BF),
            pltpu.VMEM((2, 7, BLOCK, CA[2]), BF),
            pltpu.VMEM((12, BLOCK, CB[0]), BF),
            pltpu.VMEM((12, BLOCK, CB[2]), BF),
            pltpu.VMEM((16, BLOCK, CA[2]), BF),
            pltpu.VMEM((16, BLOCK, CB[2]), BF),
            pltpu.VMEM((2, 2, BLOCK, CA[2]), BF),
            pltpu.VMEM((2, 6, BLOCK, CA[2]), BF),
            pltpu.VMEM((4, BLOCK, CB[2]), BF),
            pltpu.VMEM((4, BLOCK, CB[2]), BF),
            pltpu.VMEM((4, BLOCK, CB[2]), BF),
            pltpu.VMEM((8, BLOCK, CB[2]), BF),
            pltpu.VMEM((4, BLOCK), I32),
            pltpu.VMEM((10, 4, BLOCK), I32),
            pltpu.VMEM((5, 4, BLOCK), I32),
            pltpu.SMEM((10, 4, BLOCK), I32),
            pltpu.SMEM((5, 4, BLOCK), I32),
            pltpu.VMEM((8, 2 * BLOCK), I32),
            pltpu.VMEM((8, 3 * BLOCK), I32),
            pltpu.SMEM((8, 3 * BLOCK), I32),
            dma((12,)),
            dma((240,)),
            dma((15,)),
            dma((2, 2, 2)),
            dma((3, 4)),
            dma((3, 2, 2)),
            dma((3, 4, 2, 2)),
            dma((3, 3, 2)),
            dma((3, 2, 4)),
            dma((3, 4, 2)),
            dma((3, 4)),
            dma((4,)),
            dma((1,)),
            dma((2, 2)),
            dma((4, 2)),
            dma((3, 2)),
            dma((4,)),
        ],
        compiler_params=pltpu.CompilerParams(
            collective_id=0, has_side_effects=True, vmem_limit_bytes=67043328
        ),
    )(
        initial.reshape(4, BLOCK, D),
        held_cross,
        weights,
        need_rows.reshape(1, 16),
        tiles[0, 0],
        tile_scale[0],
        tile_src[0],
        tile_dst[0],
        tile_count,
        cross_need[0, 0].T,
        cross_tiles[0, 0],
        cross_scale[0],
        cross_src[0],
        cross_dst[0],
    )
    return pl.pallas_call(
        finish,
        out_shape=(table, table),
        in_specs=[hbm, hbm],
        out_specs=(hbm, hbm),
        scratch_shapes=[pltpu.VMEM((ROWS, D), BF)] * 2 + [dma((4,))],
    )(*out)


def solution(mesh):
    in_specs = (
        P(("comm", "dom"), None),
        P(("comm", "dom"), None),
        P(),
        P("comm", "dom", None, None),
        P("comm", "dom", None, None, None),
        P("comm", "dom", None),
        P("comm", "dom", None),
        P("comm", "dom", None),
        P("comm", "dom"),
        P("comm", "dom", None, None),
        P("comm", "dom", None, None, None),
        P("comm", "dom", None),
        P("comm", "dom", None),
        P("comm", "dom", None),
    )
    out_specs = (P(("comm", "dom"), None), P(("comm", "dom"), None))
    return jax.shard_map(
        per_device, mesh=mesh, in_specs=in_specs, out_specs=out_specs, check_vma=False
    )
```
